32 devices in a mesh: dp: 8 (over z, y), section: 4 (over x, core).
Axes of the slice: x: 2, y: 2, z: 4, core: 2. Of those that a mesh axis runs over, the one named last changes fastest.
Arguments:
- patches: bfloat16 [64, 197, 1024], P('dp'), may hold values from -6 to 6
- ln1_gain: float32 [4, 1024], P('section'), may hold values from 0.5 to 1.5
- w_qkv: bfloat16 [4, 1024, 3072], P('section'), may hold values from -1 to 1
- w_out: bfloat16 [4, 1024, 1024], P('section'), may hold values from -0.1875 to 0.1875
- ln2_gain: float32 [4, 1024], P('section'), may hold values from 0.5 to 1.5
- w_fc1: bfloat16 [4, 1024, 2048], P('section'), may hold values from -0.1875 to 0.1875
- w_fc2: bfloat16 [4, 2048, 1024], P('section'), may hold values from -0.125 to 0.125
- final_norm_gain: float32 [1024], replicated, may hold values from 0.5 to 1.5
- w_head: bfloat16 [1024, 256], replicated, may hold values from -0.1875 to 0.1875
- online_embeddings: bfloat16 [64, 256], P('dp'), may hold values from -60 to 60
- queue: bfloat16 [32768, 256], P(('dp', 'section')), may hold values from -1 to 1, as said below
- owner: int32 [64], replicated, may hold values from 0 to 63, each once
- pointer: int32 [8], P('dp'), may hold values from 0 to 4088
Outputs:
- momentum_embeddings: bfloat16 [64, 256], P('dp')
- query_loss: float32 [64], P('dp')
- total_loss: float32 [], replicated
- new_queue: bfloat16 [32768, 256], P(('dp', 'section'))
The draws below stay inside these ranges and needn't reach their ends.
Inputs may be any that keep to these rules, and one draw needn't show every extreme that they name: `queue`: every row has Euclidean norm below 1. Each value appears once: key j goes to group owner[j] // 8, so every group receives exactly 8 keys. `pointer`: first row of the group's shard where its new keys are written.
All inputs are finite; a program needn't handle non-finite values.
Results may differ from the reference program's by a relative error of at most 0.02.
Values may be sent and summed in bfloat16 or wider, within the bound.
No kernel may reach another device: no remote copies, remote signals or barrier semaphores. Data moves between devices by JAX's collectives and lax.ppermute only.
A program may use at most 128 MiB of HBM per device.

```python
import math
import jax
import jax.numpy as jnp
from jax import lax

D = 1024
HEADS = 16
HEAD_DIM = 64
FF = 2048
TOKS = 197
KDIM = 256
Q_GROUP = 4096
IMG_GROUP = 8
IMAGES = 64
QROWS = 32768
N_DP = 8
N_SECTION = 4


def draw_w_qkv(key, part):
    result = jax.random.normal(jax.random.fold_in(key, 23), (N_SECTION, D, 3 * D), jnp.float32) / D ** 0.5
    result = jnp.clip(result, -6.0 / D ** 0.5, 6.0 / D ** 0.5)
    return result.astype(jnp.bfloat16)


def queue_rows(key):
    sample_count = jax.random.normal(jax.random.fold_in(key, 11), (QROWS, KDIM), jnp.float32)
    return sample_count * jax.lax.rsqrt(jnp.sum(sample_count * sample_count, axis=1, keepdims=True) + 1.0)


def draw_queue(key, part):
    return queue_rows(key).astype(jnp.bfloat16)


def draw_online_embeddings(key, part):
    result = jnp.clip(jax.random.normal(jax.random.fold_in(key, 5), (IMAGES, KDIM), jnp.float32), -6.0, 6.0)
    return result.astype(jnp.bfloat16)


def plant(drawn, key, low, largest):
    place = [jax.random.randint(jax.random.fold_in(key, axis), (), 0, length) for axis, length in enumerate(drawn.shape)]
    main_axis = drawn.shape.index(max(drawn.shape))
    beside = place[:main_axis] + [(place[main_axis] + 1) % drawn.shape[main_axis]] + place[main_axis + 1:]
    return drawn.at[tuple(place)].set(low).at[tuple(beside)].set(largest)


def block_levels(key, shape, cuts, least, top_value):
    level = 1.0
    for position, blocks in cuts:
        heights = jax.random.uniform(jax.random.fold_in(jax.random.fold_in(key, 6), position), (blocks,), jnp.float32, least / len(cuts), top_value / len(cuts))
        level = level * jnp.repeat(jnp.exp(heights), shape[position] // blocks).reshape((-1,) + (1,) * (len(shape) - 1 - position))
    return level


def scatter_about(key, dims, scale, limit, cuts=(), kind=jnp.bfloat16):
    loudness = block_levels(key, dims, cuts, -0.22, 0.18) if cuts else 1.0
    array = jax.random.normal(key, dims, jnp.float32) * scale * loudness
    return jnp.minimum(jnp.maximum(array, -limit), limit).astype(kind)


def setup_inputs(seed: int = 0) -> dict:
    seeds = jax.random.split(jax.random.key(seed), 14)
    return {
        "patches": scatter_about(seeds[0], (IMAGES, TOKS, D), 1.0, 6.0, ((0, 8),)),
        "ln1_gain": jnp.clip(1.0 + 0.1 * jax.random.normal(seeds[1], (N_SECTION, D), jnp.float32), 0.5, 1.5),
        "w_qkv": draw_w_qkv(jax.random.fold_in(seeds[13], 71), 0),
        "w_out": scatter_about(seeds[3], (N_SECTION, D, D), D ** -0.5, 0.1875, ((0, 4),)),
        "ln2_gain": jnp.clip(1.0 + 0.1 * jax.random.normal(seeds[4], (N_SECTION, D), jnp.float32), 0.5, 1.5),
        "w_fc1": scatter_about(seeds[5], (N_SECTION, D, FF), D ** -0.5, 0.1875, ((0, 4),)),
        "w_fc2": scatter_about(seeds[6], (N_SECTION, FF, D), FF ** -0.5, 0.125, ((0, 4),)),
        "final_norm_gain": jnp.clip(1.0 + 0.1 * jax.random.normal(seeds[7], (D,), jnp.float32), 0.5, 1.5),
        "w_head": scatter_about(seeds[8], (D, KDIM), D ** -0.5, 0.1875),
        "online_embeddings": draw_online_embeddings(jax.random.fold_in(seeds[13], 71), 0),
        "queue": draw_queue(jax.random.fold_in(seeds[13], 71), 0),
        "owner": jax.random.permutation(seeds[11], IMAGES).astype(jnp.int32),
        "pointer": plant(jax.random.randint(seeds[12], (N_DP,), 0, Q_GROUP - IMG_GROUP + 1), jax.random.fold_in(seeds[12], 1), 0, Q_GROUP - IMG_GROUP).astype(jnp.int32),
    }


contrastive_sharpness = 0.2

def layer_norm(values, gain):
    center = values - lax.optimization_barrier(jnp.mean(values, axis=-1, keepdims=True))
    spread = lax.optimization_barrier(jnp.mean(center * center, axis=-1, keepdims=True))
    return center * lax.rsqrt(spread + 1e-06) * gain

def cycle_buffer(values):
    return lax.optimization_barrier(values.astype(jnp.bfloat16)).astype(jnp.float32)

def encoder_block(hidden, gain_one, qkv_weight, out_weight, gain_two, first_weight, second_weight):
    images = hidden.shape[0]
    width = hidden.shape[2]
    stream = hidden.astype(jnp.float32)
    normed = layer_norm(stream, gain_one).astype(jnp.bfloat16).reshape(images * TOKS, width)
    packed = jnp.dot(normed, qkv_weight, preferred_element_type=jnp.float32)
    packed = cycle_buffer(packed).reshape(images, TOKS, 3, HEADS, HEAD_DIM)
    similarity_matrix = jnp.einsum('bqhd,bkhd->bhqk', packed[:, :, 0], packed[:, :, 1]) / math.sqrt(HEAD_DIM)
    peak = lax.optimization_barrier(jnp.max(similarity_matrix, axis=-1, keepdims=True))
    expo = jnp.exp(similarity_matrix - peak)
    probs = cycle_buffer(expo / lax.optimization_barrier(jnp.sum(expo, axis=-1, keepdims=True)))
    context = jnp.einsum('bhqk,bkhd->bqhd', probs, packed[:, :, 2])
    context = context.astype(jnp.bfloat16).reshape(images * TOKS, width)
    stream = stream + jnp.dot(context, out_weight, preferred_element_type=jnp.float32).reshape(images, TOKS, width)
    normed = layer_norm(stream, gain_two).astype(jnp.bfloat16).reshape(images * TOKS, width)
    inner = jax.nn.gelu(jnp.dot(normed, first_weight, preferred_element_type=jnp.float32), approximate=False)
    inner = inner.astype(jnp.bfloat16)
    stream = stream + jnp.dot(inner, second_weight, preferred_element_type=jnp.float32).reshape(images, TOKS, width)
    return stream.astype(jnp.bfloat16)

def key_head(class_rows, final_norm_gain, w_head):
    normed = layer_norm(class_rows.astype(jnp.float32), final_norm_gain).astype(jnp.bfloat16)
    projected = jnp.dot(normed, w_head, preferred_element_type=jnp.float32)
    scale = lax.rsqrt(1.0 + lax.optimization_barrier(jnp.sum(projected * projected, axis=1, keepdims=True)))
    return (projected * scale).astype(jnp.bfloat16)

def reference(patches, ln1_gain, w_qkv, w_out, ln2_gain, w_fc1, w_fc2, final_norm_gain, w_head, online_embeddings, queue, owner, pointer):

    def encode_group(images):
        hidden = images
        for layer_section in range(N_SECTION):
            hidden = encoder_block(hidden, ln1_gain[layer_section], w_qkv[layer_section], w_out[layer_section], ln2_gain[layer_section], w_fc1[layer_section], w_fc2[layer_section])
        return key_head(hidden[:, 0, :], final_norm_gain, w_head)
    momentum_embeddings = lax.map(encode_group, patches.reshape(N_DP, IMG_GROUP, TOKS, D)).reshape(IMAGES, KDIM)
    matching_similarity = lax.optimization_barrier(jnp.sum(online_embeddings.astype(jnp.float32) * momentum_embeddings.astype(jnp.float32), axis=1)) / contrastive_sharpness

    def score_group(sample_count):
        similarity_matrix = jnp.dot(online_embeddings, sample_count.T, preferred_element_type=jnp.float32) / contrastive_sharpness
        peak = lax.optimization_barrier(jnp.max(similarity_matrix, axis=1))
        return (peak, lax.optimization_barrier(jnp.sum(jnp.exp(similarity_matrix - peak[:, None]), axis=1)))
    peaks, totals = lax.map(score_group, queue.reshape(N_DP, Q_GROUP, KDIM))
    top = lax.optimization_barrier(jnp.max(peaks, axis=0))
    negative = top + jnp.log(lax.optimization_barrier(jnp.sum(totals * jnp.exp(peaks - top[None, :]), axis=0)))
    larger = jnp.maximum(negative, matching_similarity)
    query_loss = larger + jnp.log(jnp.exp(negative - larger) + jnp.exp(matching_similarity - larger)) - matching_similarity
    total_loss = jnp.sum(query_loss) / IMAGES
    order = jnp.zeros((IMAGES,), jnp.int32).at[owner].set(jnp.arange(IMAGES, dtype=jnp.int32))
    entries = momentum_embeddings[order].reshape(N_DP, IMG_GROUP, KDIM)

    def enqueue(pieces):
        sample_count, fresh, start = pieces
        return lax.dynamic_update_slice_in_dim(sample_count, fresh, start.astype(jnp.int32), 0)
    new_queue = lax.map(enqueue, (queue.reshape(N_DP, Q_GROUP, KDIM), entries, pointer)).reshape(QROWS, KDIM)
    return (momentum_embeddings, query_loss, total_loss, new_queue)
```

```python
import functools
import math

import jax
import jax.numpy as jnp
from jax import lax
from jax.experimental import pallas as pl
from jax.experimental.pallas import tpu as pltpu
from jax.sharding import PartitionSpec as P

F32 = jnp.float32
BF16 = jnp.bfloat16
HEAD_DIM = 64
LANES = 128
WIDE = 256
SHARPNESS = 0.2
HOP = 2


def layer_norm(values, gain):
    center = values - jnp.mean(values, axis=-1, keepdims=True)
    spread = jnp.mean(center * center, axis=-1, keepdims=True)
    return center * lax.rsqrt(spread + 1e-06) * gain


def mm(left, right):
    return jnp.dot(left, right, preferred_element_type=F32)


def mm_t(left, right):
    return lax.dot_general(left, right, (((1,), (1,)), ((), ())), preferred_element_type=F32)


def encode(x_ref, g1, wqkv, wout, g2, wfc1, wfc2, out_ref, norm, qkv, ctx, res, act, toks):
    rows, width = norm.shape
    ff = wfc1.shape[1]
    norm[...] = layer_norm(x_ref[...].astype(F32), g1[...]).astype(BF16)
    quad = WIDE // HEAD_DIM
    pair = LANES // HEAD_DIM
    scale = 1.0 / math.sqrt(HEAD_DIM)
    lane = lax.broadcasted_iota(jnp.int32, (rows, LANES), 1) // HEAD_DIM
    keep = lax.broadcasted_iota(jnp.int32, (rows, rows), 1) < toks

    def project(j):
        for part in range(3):
            o = part * width + j * WIDE
            y = mm(norm[...], wqkv[:, o : o + WIDE])
            if part == 0:
                y = y.astype(BF16).astype(F32) * scale
            qkv[:, o : o + WIDE] = y.astype(BF16)

    def scores(j):
        found = []
        for h in range(quad):
            o = j * WIDE + (h // pair) * LANES
            q = qkv[:, o : o + LANES]
            q = jnp.where(lane == h % pair, q, jnp.zeros_like(q))
            found.append(mm_t(q, qkv[:, width + o : width + o + LANES]))
        return found

    def soften(found):
        out = []
        for s in found:
            s = jnp.where(keep, s, -1e30)
            out.append(jnp.exp(s - jnp.max(s, axis=-1, keepdims=True)).astype(BF16))
        return out

    def mix(j, weights):
        ones = jnp.ones((rows, LANES), BF16)
        for half in range(quad // pair):
            o = j * WIDE + half * LANES
            v = jnp.concatenate([qkv[:, 2 * width + o : 2 * width + o + LANES], ones], axis=1)
            got = None
            for i in range(pair):
                y = mm(weights[half * pair + i], v)
                y = y[:, :LANES] / y[:, LANES:]
                got = y if got is None else jnp.where(lane == i, y, got)
            ctx[:, o : o + LANES] = got.astype(BF16)

    groups = width // WIDE
    project(0)
    found = scores(0)
    for j in range(groups):
        if j + 1 < groups:
            project(j + 1)
        mix(j, soften(found))
        if j + 1 < groups:
            found = scores(j + 1)
    for n in range(0, width, WIDE):
        res[:, n : n + WIDE] = x_ref[:, n : n + WIDE].astype(F32) + mm(ctx[...], wout[:, n : n + WIDE])
    norm[...] = layer_norm(res[...], g2[...]).astype(BF16)
    for n in range(0, ff, WIDE):
        t = mm(norm[...], wfc1[:, n : n + WIDE])
        t = 0.5 * t * (1.0 + lax.erf(t * (1.0 / math.sqrt(2.0))))
        act[:, n : n + WIDE] = t.astype(BF16)
    for n in range(0, width, WIDE):
        out_ref[:, n : n + WIDE] = (res[:, n : n + WIDE] + mm(act[...], wfc2[:, n : n + WIDE])).astype(BF16)


def tick_kernel(
    place, patch, came, g1, wqkv, wout, g2, wfc1, wfc2, out_ref, cls_ref, x_s, norm, qkv, ctx, res, act, *, tick, toks
):
    section = place[0]
    images = place[1]
    step = tick - HOP * section

    @pl.when(jnp.logical_and(step >= 0, step < images))
    def _():
        @pl.when(section == 0)
        def _():
            x_s[...] = jnp.zeros_like(x_s)
            x_s[0:toks, :] = patch[0]

        @pl.when(section != 0)
        def _():
            x_s[...] = came[...]

        encode(x_s, g1, wqkv, wout, g2, wfc1, wfc2, out_ref, norm, qkv, ctx, res, act, toks)
        cls_ref[...] = out_ref[0:8, :]


def run_tick(tick, place, patches, came, weights):
    images, toks, width = patches.shape
    rows = came.shape[0]
    ff = weights[4].shape[1]
    whole = pl.BlockSpec(memory_space=pltpu.VMEM)
    which = min(tick, images - 1)
    return pl.pallas_call(
        functools.partial(tick_kernel, tick=tick, toks=toks),
        out_shape=(jax.ShapeDtypeStruct((rows, width), BF16), jax.ShapeDtypeStruct((8, width), BF16)),
        in_specs=[pl.BlockSpec(memory_space=pltpu.SMEM), whole, whole] + [whole] * 6,
        out_specs=(whole, whole),
        scratch_shapes=[
            pltpu.VMEM((rows, width), BF16),
            pltpu.VMEM((rows, width), BF16),
            pltpu.VMEM((rows, 3 * width), BF16),
            pltpu.VMEM((rows, width), BF16),
            pltpu.VMEM((rows, width), F32),
            pltpu.VMEM((rows, ff), BF16),
        ],
        compiler_params=pltpu.CompilerParams(vmem_limit_bytes=30 * 2**20),
        name="block",
    )(place, lax.slice_in_dim(patches, which, which + 1, axis=0), came, *weights)


def lse_kernel(query, queue, out_ref):
    s = mm_t(query[...], queue[...]) * (1.0 / SHARPNESS)
    peak = jnp.max(s, axis=1, keepdims=True)
    out_ref[...] = peak + jnp.log(jnp.sum(jnp.exp(s - peak), axis=1, keepdims=True))


def head_kernel(*refs, images, extra):
    cls = refs[:images]
    gain, head, lse, out_ref, gather = refs[images:]
    for i in range(images):
        gather[i : i + 1, :] = cls[i][0:1, :].astype(F32)
    normed = layer_norm(gather[...], gain[...]).astype(BF16)
    z = mm(normed, head[...])
    z = z * lax.rsqrt(1.0 + jnp.sum(z * z, axis=1, keepdims=True))
    kd = z.shape[1]
    peers, rows, lanes = out_ref.shape
    parts = [z[:, o : o + lanes] for o in range(0, kd, lanes)]
    high = lse[...].astype(BF16).astype(F32)
    mid = (lse[...] - high).astype(BF16).astype(F32)
    low = lse[...] - high - mid
    parts += [high, mid, low]
    used = sum(p.shape[0] for p in parts)
    parts.append(jnp.zeros((rows - used, lanes), F32))
    block = jnp.concatenate(parts, axis=0).astype(BF16)
    out_ref[...] = jnp.broadcast_to(block[None], out_ref.shape)


def final_kernel(
    place, got, query, owner, queue_in, keys_ref, loss_ref, total_ref, queue_ref, window, sem, *, images, extra, kd
):
    section, _, group, groups, sections, start = [place[i] for i in range(6)]
    share = queue_ref.shape[0]
    local = start - section * share
    span = window.shape[0]
    base = jnp.clip((local // 16) * 16, 0, share - span)
    base = pl.multiple_of(base, 16)
    fetch = pltpu.make_async_copy(queue_ref.at[pl.ds(base, span), :], window, sem)
    fetch.start()
    peers, rows, lanes = got.shape
    halves = kd // lanes
    last = peers // query.shape[0] * images
    count = query.shape[0]
    n_sec = peers * images // count
    pieces = []
    for g in range(count // images):
        src = g * n_sec + n_sec - 1
        one = got[src].astype(F32)
        pieces.append(jnp.concatenate([one[h * images : (h + 1) * images] for h in range(halves)], axis=1))
    keys = jnp.concatenate(pieces, axis=0)
    keys16 = keys.astype(BF16)
    msgs = got[...].astype(F32)
    off = halves * images
    lse = msgs[:, off : off + extra, :] + msgs[:, off + extra : off + 2 * extra, :] + msgs[:, off + 2 * extra : off + 3 * extra, :]
    peak = jnp.max(lse, axis=0)
    negative = peak + jnp.log(jnp.sum(jnp.exp(lse - peak[None]), axis=0))
    square = mm_t(query[...], keys16)
    r = lax.broadcasted_iota(jnp.int32, square.shape, 0)
    c = lax.broadcasted_iota(jnp.int32, square.shape, 1)
    positive = jnp.sum(jnp.where(r == c, square, 0.0), axis=0, keepdims=True) * (1.0 / SHARPNESS)
    positive = jnp.pad(positive, ((0, 0), (0, lanes - count)))
    larger = jnp.maximum(negative, positive)
    loss = larger + jnp.log(jnp.exp(negative - larger) + jnp.exp(positive - larger)) - positive
    lane = lax.broadcasted_iota(jnp.int32, loss.shape, 1)
    total_ref[...] = jnp.sum(jnp.where(lane < count, loss, 0.0), axis=1, keepdims=True) * (1.0 / count)
    turned = pltpu.roll(jnp.broadcast_to(loss, (8, lanes)), lanes - group * images, 1)
    loss_ref[...] = turned[0:1, 0:images]
    mine = got[group * n_sec + n_sec - 1].astype(F32)
    keys_ref[...] = jnp.concatenate([mine[h * images : (h + 1) * images] for h in range(halves)], axis=1).astype(BF16)
    row = lax.broadcasted_iota(jnp.int32, (span, count), 0) + (base - local)
    slot = owner[...] - group * images
    pick = jnp.logical_and(row == slot, jnp.logical_and(slot >= 0, slot < images))
    fresh = mm(pick.astype(F32).astype(BF16), keys16)
    hit = jnp.sum(pick.astype(F32), axis=1, keepdims=True) > 0.5
    fetch.wait()
    window[...] = jnp.where(hit, fresh, window[...].astype(F32)).astype(BF16)
    back = pltpu.make_async_copy(window, queue_ref.at[pl.ds(base, span), :], sem)
    back.start()
    back.wait()


def on_device(
    patches,
    ln1_gain,
    w_qkv,
    w_out,
    ln2_gain,
    w_fc1,
    w_fc2,
    final_norm_gain,
    w_head,
    online_embeddings,
    queue,
    owner,
    pointer,
):
    sections = lax.axis_size("section")
    groups = lax.axis_size("dp")
    section = lax.axis_index("section").astype(jnp.int32)
    group = lax.axis_index("dp").astype(jnp.int32)
    images, toks, width = patches.shape
    kd = w_head.shape[1]
    peers = sections * groups
    count = groups * images
    rows = -(-toks // 16) * 16
    whole = pl.BlockSpec(memory_space=pltpu.VMEM)
    smem = pl.BlockSpec(memory_space=pltpu.SMEM)
    hbm = pl.BlockSpec(memory_space=pl.ANY)
    place = jnp.stack([section, jnp.int32(images), group, jnp.int32(groups), jnp.int32(sections), pointer[0]])

    query = online_embeddings
    hop = 1
    while hop < groups:
        other = lax.ppermute(query, "dp", [(s, s ^ hop) for s in range(groups)])
        upper = (group & hop) != 0
        query = jnp.concatenate([jnp.where(upper, other, query), jnp.where(upper, query, other)], axis=0)
        hop *= 2

    lse = pl.pallas_call(
        lse_kernel,
        out_shape=jax.ShapeDtypeStruct((count, 1), F32),
        in_specs=[whole, whole],
        out_specs=whole,
        name="lse",
    )(query, queue)

    weights = (ln1_gain, w_qkv[0], w_out[0], ln2_gain, w_fc1[0], w_fc2[0])
    came = jnp.zeros((rows, width), BF16)
    sent = came
    marks = []
    ticks = images + HOP * (sections - 1)
    chain = [(s, s + 1) for s in range(sections - 1)]
    for tick in range(ticks):
        if tick >= 1 and tick + 1 < ticks:
            nxt = lax.ppermute(sent, "section", chain)
        else:
            nxt = came
        sent, mark = run_tick(tick, place, patches, came, weights)
        marks.append(mark)
        came = nxt
    marks = marks[-images:]

    extra = -(-count // LANES)
    flat = jnp.pad(lse.reshape(1, count), ((0, 0), (0, extra * LANES - count))).reshape(extra, LANES)
    height = -(-(kd // LANES * images + 3 * extra) // 8) * 8
    message = pl.pallas_call(
        functools.partial(head_kernel, images=images, extra=extra),
        out_shape=jax.ShapeDtypeStruct((peers, height, LANES), BF16),
        in_specs=[whole] * (images + 3),
        out_specs=whole,
        scratch_shapes=[pltpu.VMEM((images, width), F32)],
        name="head",
    )(*marks, final_norm_gain.reshape(1, width), w_head, flat)
    got = lax.all_to_all(message, ("dp", "section"), 0, 0, tiled=True)

    keys, loss, total, new_queue = pl.pallas_call(
        functools.partial(final_kernel, images=images, extra=extra, kd=kd),
        out_shape=(
            jax.ShapeDtypeStruct((images, kd), BF16),
            jax.ShapeDtypeStruct((1, images), F32),
            jax.ShapeDtypeStruct((1, 1), F32),
            jax.ShapeDtypeStruct(queue.shape, BF16),
        ),
        in_specs=[smem, whole, whole, whole, hbm],
        out_specs=(whole, whole, whole, hbm),
        scratch_shapes=[pltpu.VMEM((32, kd), BF16), pltpu.SemaphoreType.DMA],
        input_output_aliases={4: 3},
        name="final",
    )(place, got, query, owner.reshape(1, count), queue)
    return keys, loss.reshape(images), total.reshape(()), new_queue


def solution(mesh):
    placed = (
        P("dp", None, None),
        P("section", None),
        P("section", None, None),
        P("section", None, None),
        P("section", None),
        P("section", None, None),
        P("section", None, None),
        P(),
        P(),
        P("dp", None),
        P(("dp", "section"), None),
        P(),
        P("dp"),
    )
    return jax.shard_map(
        on_device,
        mesh=mesh,
        in_specs=placed,
        out_specs=(P("dp", None), P("dp"), P(), P(("dp", "section"), None)),
        check_vma=False,
    )
```

```python
import functools
import math

import jax
import jax.numpy as jnp
from jax import lax
from jax.experimental import pallas as pl
from jax.experimental.pallas import tpu as pltpu
from jax.sharding import PartitionSpec as P

F32 = jnp.float32
BF16 = jnp.bfloat16
HEAD_DIM = 64
LANES = 128
WIDE = 256
SHARPNESS = 0.2
HOP = 2
UNROLL = 2


def layer_norm(values, gain):
    center = values - jnp.mean(values, axis=-1, keepdims=True)
    spread = jnp.mean(center * center, axis=-1, keepdims=True)
    return center * lax.rsqrt(spread + 1e-06) * gain


def mm(left, right):
    return jnp.dot(left, right, preferred_element_type=F32)


def mm_t(left, right):
    return lax.dot_general(left, right, (((1,), (1,)), ((), ())), preferred_element_type=F32)


def attention_tools(rows, toks):
    pair = LANES // HEAD_DIM
    lane = lax.broadcasted_iota(jnp.int32, (rows, LANES), 1) // HEAD_DIM
    keep = lax.broadcasted_iota(jnp.int32, (rows, rows), 1) < toks
    return pair, lane, keep


def encode(wqkv, wout, g2, wfc1, wfc2, out_ref, norm, qkv, ctx, res, act, toks, ready=None):
    rows, width = norm.shape
    ff = wfc1.shape[1]
    quad = WIDE // HEAD_DIM
    pair, lane, keep = attention_tools(rows, toks)
    scale = 1.0 / math.sqrt(HEAD_DIM)
    ready = ready or (lambda k: None)

    def project(j):
        for part in range(3):
            o = part * width + j * WIDE
            y = mm(norm[...], wqkv[:, o : o + WIDE])
            if part == 0:
                y = y * scale
            qkv[:, o : o + WIDE] = y.astype(BF16)

    def scores(j):
        found = []
        for h in range(quad):
            o = j * WIDE + (h // pair) * LANES
            q = qkv[:, o : o + LANES]
            q = jnp.where(lane == h % pair, q, jnp.zeros_like(q))
            found.append(mm_t(q, qkv[:, width + o : width + o + LANES]))
        return found

    def soften(found):
        out = []
        for s in found:
            s = jnp.where(keep, s, -1e30)
            out.append(jnp.exp(s - jnp.max(s, axis=-1, keepdims=True)).astype(BF16))
        return out

    def mix(j, weights):
        ones = jnp.ones((rows, LANES), BF16)
        for half in range(quad // pair):
            o = j * WIDE + half * LANES
            v = jnp.concatenate([qkv[:, 2 * width + o : 2 * width + o + LANES], ones], axis=1)
            got = None
            for i in range(pair):
                y = mm(weights[half * pair + i], v)
                y = y[:, :LANES] / y[:, LANES:]
                got = y if got is None else jnp.where(lane == i, y, got)
            ctx[:, o : o + LANES] = got.astype(BF16)

    groups = width // WIDE
    ready(0)
    project(0)
    found = scores(0)
    for j in range(groups):
        if j + 1 < groups:
            project(j + 1)
        mix(j, soften(found))
        if j + 1 < groups:
            found = scores(j + 1)
    ready(1)
    for n in range(0, width, WIDE):
        res[:, n : n + WIDE] += mm(ctx[...], wout[:, n : n + WIDE])
    norm[...] = layer_norm(res[...], g2[...]).astype(BF16)
    ready(2)
    for n in range(0, ff, WIDE):
        t = mm(norm[...], wfc1[:, n : n + WIDE])
        t = 0.5 * t * (1.0 + lax.erf(t * (1.0 / math.sqrt(2.0))))
        act[:, n : n + WIDE] = t.astype(BF16)
    ready(3)
    for n in range(0, width, WIDE):
        out_ref[:, n : n + WIDE] = (res[:, n : n + WIDE] + mm(act[...], wfc2[:, n : n + WIDE])).astype(BF16)


def encode_class(x_ref, g1, wqkv, wout, g2, wfc1, wfc2, norm, qkv, toks):
    rows, width = norm.shape
    heads = width // HEAD_DIM
    scale = 1.0 / math.sqrt(HEAD_DIM)
    norm[...] = layer_norm(x_ref[...].astype(F32), g1[...]).astype(BF16)
    q = mm(norm[0:16, :], wqkv[:, 0:width])[0:1, :] * scale
    own = lax.broadcasted_iota(jnp.int32, (heads, width), 1) // HEAD_DIM
    own = own == lax.broadcasted_iota(jnp.int32, (heads, width), 0)
    q = jnp.where(own, jnp.broadcast_to(q, (heads, width)), 0.0).astype(BF16)
    for o in range(width, 2 * width, WIDE):
        qkv[:, o : o + WIDE] = mm(norm[...], wqkv[:, o : o + WIDE]).astype(BF16)
    s = mm_t(q, qkv[:, width : 2 * width])
    s = jnp.where(lax.broadcasted_iota(jnp.int32, s.shape, 1) < toks, s, -1e30)
    e = jnp.exp(s - jnp.max(s, axis=-1, keepdims=True))
    p = (e / jnp.sum(e, axis=-1, keepdims=True)).astype(BF16)
    mixed = mm(p, norm[...]).astype(BF16)
    c = mm(mixed, wqkv[:, 2 * width : 3 * width])
    c = jnp.sum(jnp.where(own, c, 0.0), axis=0, keepdims=True)
    c = jnp.broadcast_to(c, (8, width)).astype(BF16)
    r = x_ref[0:8, :].astype(F32)[0:1, :] + mm(c, wout[...])
    n = layer_norm(r, g2[...]).astype(BF16)
    t = mm(n, wfc1[...])
    t = 0.5 * t * (1.0 + lax.erf(t * (1.0 / math.sqrt(2.0))))
    return (r + mm(t.astype(BF16), wfc2[...]))[0:1, :].astype(BF16).astype(F32)


def first_kernel(
    patch_hbm, wqkv_hbm, wout_hbm, wfc1_hbm, wfc2_hbm, g1, g2,
    out_ref, turned, wqkv, wout, wfc1, wfc2, marks, blank, count,
    flat, norm, qkv, ctx, res, act, sems, *, images, toks,
):
    copies = [
        pltpu.make_async_copy(a, b, sems.at[k])
        for k, (a, b) in enumerate(((wqkv_hbm, wqkv), (wout_hbm, wout), (wfc1_hbm, wfc1), (wfc2_hbm, wfc2)))
    ]
    total = toks * images
    fetch = pltpu.make_async_copy(patch_hbm, flat.at[0:total, :], sems.at[4])
    fetch.start()
    for c in copies:
        c.start()
    section = lax.axis_index("section")
    marks[...] = jnp.zeros_like(marks)
    blank[...] = jnp.zeros_like(blank)
    count[0] = 1

    @pl.when(section == 0)
    def _():
        span = flat.shape[0]
        flat[total:span, :] = jnp.zeros((span - total, flat.shape[1]), BF16)
        fetch.wait()
        take = WIDE // images
        r = lax.broadcasted_iota(jnp.int32, (WIDE, WIDE), 0)
        c = lax.broadcasted_iota(jnp.int32, (WIDE, WIDE), 1)
        order = (c == (r % take) * images + r // take).astype(F32).astype(BF16)
        rows = turned.shape[1]
        for k in range(0, rows, take):
            got = mm(order, flat[k * images : k * images + WIDE, :]).astype(BF16)
            size = min(take, rows - k)
            for i in range(images):
                turned[i, k : k + size, :] = got[i * take : i * take + size, :]
        x = turned[0].astype(F32)
        res[...] = x
        norm[...] = layer_norm(x, g1[...]).astype(BF16)
        encode(wqkv, wout, g2, wfc1, wfc2, out_ref, norm, qkv, ctx, res, act, toks, ready=lambda k: copies[k].wait())

    @pl.when(section != 0)
    def _():
        fetch.wait()
        for c in copies:
            c.wait()


def first_tick(patches, weights, rows):
    images, toks, width = patches.shape
    g1, wqkv, wout, g2, wfc1, wfc2 = weights
    ff = wfc1.shape[1]
    whole = pl.BlockSpec(memory_space=pltpu.VMEM)
    hbm = pl.BlockSpec(memory_space=pl.ANY)
    span = -(-rows * images // WIDE) * WIDE
    return pl.pallas_call(
        functools.partial(first_kernel, images=images, toks=toks),
        out_shape=(
            pltpu.VMEM((rows, width), BF16),
            pltpu.VMEM((images, rows, width), BF16),
            pltpu.VMEM(wqkv.shape, BF16),
            pltpu.VMEM(wout.shape, BF16),
            pltpu.VMEM(wfc1.shape, BF16),
            pltpu.VMEM(wfc2.shape, BF16),
            pltpu.VMEM((images, width), F32),
            pltpu.VMEM((rows, width), BF16),
            pltpu.SMEM((1,), jnp.int32),
        ),
        in_specs=[hbm] * 5 + [whole] * 2,
        out_specs=(whole,) * 8 + (pl.BlockSpec(memory_space=pltpu.SMEM),),
        scratch_shapes=[
            pltpu.VMEM((span, width), BF16),
            pltpu.VMEM((rows, width), BF16),
            pltpu.VMEM((rows, 3 * width), BF16),
            pltpu.VMEM((rows, width), BF16),
            pltpu.VMEM((rows, width), F32),
            pltpu.VMEM((rows, ff), BF16),
            pltpu.SemaphoreType.DMA((5,)),
        ],
        compiler_params=pltpu.CompilerParams(vmem_limit_bytes=14 * 2**20),
        name="first",
    )(far(patches.transpose(1, 0, 2).reshape(toks * images, width)), far(wqkv), far(wout), far(wfc1), far(wfc2), g1, g2)


def tick_kernel(
    tick, turned, came, marks_in, g1, wqkv, wout, g2, wfc1, wfc2, out_ref, marks, after, norm, qkv, ctx, res, act, *, toks
):
    after[0] = tick[0] + 1
    section = lax.axis_index("section")
    last = lax.axis_size("section") - 1
    images = turned.shape[0]
    step = tick[0] - HOP * section
    active = jnp.logical_and(step >= 0, step < images)

    def start(x):
        res[...] = x
        norm[...] = layer_norm(x, g1[...]).astype(BF16)

    @pl.when(jnp.logical_and(active, section != last))
    def _():
        @pl.when(section == 0)
        def _():
            start(turned[step].astype(F32))

        @pl.when(section != 0)
        def _():
            start(came[...].astype(F32))

        encode(wqkv, wout, g2, wfc1, wfc2, out_ref, norm, qkv, ctx, res, act, toks)

    @pl.when(jnp.logical_and(active, section == last))
    def _():
        marks[pl.ds(step, 1), :] = encode_class(came, g1, wqkv, wout, g2, wfc1, wfc2, norm, qkv, toks)


def hold(x):
    return pltpu.with_memory_space_constraint(x, pltpu.VMEM)


def far(x):
    return pltpu.with_memory_space_constraint(x, pltpu.HBM)


def held_weights(weights):
    g1, wqkv, wout, g2, wfc1, wfc2 = weights
    return g1, hold(wqkv), hold(wout), g2, hold(wfc1), hold(wfc2)


def run_tick(tick, turned, came, marks, weights, toks):
    rows, width = came.shape
    ff = weights[4].shape[1]
    whole = pl.BlockSpec(memory_space=pltpu.VMEM)
    return pl.pallas_call(
        functools.partial(tick_kernel, toks=toks),
        out_shape=(pltpu.VMEM((rows, width), BF16), pltpu.VMEM(marks.shape, F32), pltpu.SMEM((1,), jnp.int32)),
        in_specs=[pl.BlockSpec(memory_space=pltpu.SMEM)] + [whole] * 9,
        out_specs=(whole, whole, pl.BlockSpec(memory_space=pltpu.SMEM)),
        scratch_shapes=[
            pltpu.VMEM((rows, width), BF16),
            pltpu.VMEM((rows, 3 * width), BF16),
            pltpu.VMEM((rows, width), BF16),
            pltpu.VMEM((rows, width), F32),
            pltpu.VMEM((rows, ff), BF16),
        ],
        input_output_aliases={3: 1},
        compiler_params=pltpu.CompilerParams(vmem_limit_bytes=12 * 2**20),
        name="block",
    )(tick, hold(turned), hold(came), hold(marks), *held_weights(weights))


def merge_kernel(left, right, out_ref):
    half = left.shape[0]
    out_ref[0:half, :] = left[...]
    out_ref[half : 2 * half, :] = right[...]


def merge(left, right):
    whole = pl.BlockSpec(memory_space=pltpu.VMEM)
    return pl.pallas_call(
        merge_kernel,
        out_shape=pltpu.VMEM((2 * left.shape[0], left.shape[1]), left.dtype),
        in_specs=[whole, whole],
        out_specs=whole,
        compiler_params=pltpu.CompilerParams(vmem_limit_bytes=2**20),
        name="merge",
    )(left, right)


def lse_kernel(swapped, queue_hbm, out_ref, query_ref, copy_ref, ordered, queue, sems, *, images):
    fetch = pltpu.make_async_copy(queue_hbm, queue, sems.at[0])
    fetch.start()
    group = lax.axis_index("dp")
    count = swapped.shape[0]
    ordered[...] = jnp.zeros_like(ordered)
    for b in range(count // images):
        place = pl.multiple_of(jnp.bitwise_xor(group, b) * images, images)
        ordered[pl.ds(place, images), :] = swapped[b * images : (b + 1) * images, :].astype(F32)
    query_ref[...] = ordered[0:count, :].astype(BF16)
    fetch.wait()
    back = pltpu.make_async_copy(queue, copy_ref, sems.at[1])
    back.start()
    lanes = out_ref.shape[1]
    for k in range(out_ref.shape[0]):
        s = mm_t(queue[...], ordered[k * lanes : (k + 1) * lanes, :].astype(BF16)) * (1.0 / SHARPNESS)
        peak = jnp.max(s, axis=0, keepdims=True)
        out_ref[k : k + 1, :] = peak + jnp.log(jnp.sum(jnp.exp(s - peak), axis=0, keepdims=True))
    back.wait()


def head_kernel(came, marks, g1, wqkv, wout, g2, wfc1, wfc2, gain, head, lse, out_ref, found, norm, qkv, *, toks):
    images = found.shape[0]

    @pl.when(lax.axis_index("section") == lax.axis_size("section") - 1)
    def _():
        found[...] = marks[...]
        found[images - 1 : images, :] = encode_class(came, g1, wqkv, wout, g2, wfc1, wfc2, norm, qkv, toks)

    @pl.when(lax.axis_index("section") != lax.axis_size("section") - 1)
    def _():
        found[...] = jnp.zeros_like(found)

    normed = layer_norm(found[...], gain[...]).astype(BF16)
    z = mm(normed, head[...])
    z = z * lax.rsqrt(1.0 + jnp.sum(z * z, axis=1, keepdims=True))
    kd = z.shape[1]
    peers, rows, lanes = out_ref.shape
    parts = [z[:, o : o + lanes] for o in range(0, kd, lanes)]
    high = lse[...].astype(BF16).astype(F32)
    mid = (lse[...] - high).astype(BF16).astype(F32)
    low = lse[...] - high - mid
    parts += [high, mid, low]
    used = sum(p.shape[0] for p in parts)
    if rows > used:
        parts.append(jnp.zeros((rows - used, lanes), F32))
    block = jnp.concatenate(parts, axis=0).astype(BF16)
    out_ref[...] = jnp.broadcast_to(block[None], out_ref.shape)


def final_kernel(
    pointer, got, query, owner, queue_in, keys_ref, loss_ref, total_ref, queue_ref, window, sem, *, images, extra, kd
):
    section = lax.axis_index("section")
    group = lax.axis_index("dp")
    start = pointer[0]
    share = queue_ref.shape[0]
    local = start - section * share
    span = window.shape[0]
    base = jnp.clip((local // 16) * 16, 0, share - span)
    base = pl.multiple_of(base, 16)
    fetch = pltpu.make_async_copy(queue_ref.at[pl.ds(base, span), :], window, sem)
    fetch.start()
    peers, rows, lanes = got.shape
    halves = kd // lanes
    last = peers // query.shape[0] * images
    count = query.shape[0]
    n_sec = peers * images // count
    pieces = []
    for g in range(count // images):
        src = g * n_sec + n_sec - 1
        one = got[src].astype(F32)
        pieces.append(jnp.concatenate([one[h * images : (h + 1) * images] for h in range(halves)], axis=1))
    keys = jnp.concatenate(pieces, axis=0)
    keys16 = keys.astype(BF16)
    msgs = got[...].astype(F32)
    off = halves * images
    lse = msgs[:, off : off + extra, :] + msgs[:, off + extra : off + 2 * extra, :] + msgs[:, off + 2 * extra : off + 3 * extra, :]
    peak = jnp.max(lse, axis=0)
    negative = peak + jnp.log(jnp.sum(jnp.exp(lse - peak[None]), axis=0))
    square = mm_t(query[...], keys16)
    r = lax.broadcasted_iota(jnp.int32, square.shape, 0)
    c = lax.broadcasted_iota(jnp.int32, square.shape, 1)
    positive = jnp.sum(jnp.where(r == c, square, 0.0), axis=0, keepdims=True) * (1.0 / SHARPNESS)
    positive = jnp.pad(positive, ((0, 0), (0, lanes - count)))
    larger = jnp.maximum(negative, positive)
    loss = larger + jnp.log(jnp.exp(negative - larger) + jnp.exp(positive - larger)) - positive
    lane = lax.broadcasted_iota(jnp.int32, loss.shape, 1)
    total_ref[...] = jnp.sum(jnp.where(lane < count, loss, 0.0), axis=1, keepdims=True) * (1.0 / count)
    turned = pltpu.roll(jnp.broadcast_to(loss, (8, lanes)), lanes - group * images, 1)
    loss_ref[...] = turned[0:1, 0:images]
    mine = got[group * n_sec + n_sec - 1].astype(F32)
    keys_ref[...] = jnp.concatenate([mine[h * images : (h + 1) * images] for h in range(halves)], axis=1).astype(BF16)
    row = lax.broadcasted_iota(jnp.int32, (span, count), 0) + (base - local)
    slot = owner[...] - group * images
    pick = jnp.logical_and(row == slot, jnp.logical_and(slot >= 0, slot < images))
    fresh = mm(pick.astype(F32).astype(BF16), keys16)
    hit = jnp.sum(pick.astype(F32), axis=1, keepdims=True) > 0.5
    fetch.wait()
    window[...] = jnp.where(hit, fresh, window[...].astype(F32)).astype(BF16)
    back = pltpu.make_async_copy(window, queue_ref.at[pl.ds(base, span), :], sem)
    back.start()
    back.wait()


def on_device(
    patches,
    ln1_gain,
    w_qkv,
    w_out,
    ln2_gain,
    w_fc1,
    w_fc2,
    final_norm_gain,
    w_head,
    online_embeddings,
    queue,
    owner,
    pointer,
):
    sections = lax.axis_size("section")
    groups = lax.axis_size("dp")
    section = lax.axis_index("section").astype(jnp.int32)
    group = lax.axis_index("dp").astype(jnp.int32)
    images, toks, width = patches.shape
    kd = w_head.shape[1]
    peers = sections * groups
    count = groups * images
    rows = -(-toks // 16) * 16
    whole = pl.BlockSpec(memory_space=pltpu.VMEM)
    smem = pl.BlockSpec(memory_space=pltpu.SMEM)
    hbm = pl.BlockSpec(memory_space=pl.ANY)

    query = online_embeddings
    hop = 1
    while hop < groups:
        query = merge(query, lax.ppermute(query, "dp", [(k, k ^ hop) for k in range(groups)]))
        hop *= 2
    extra = -(-count // LANES)
    lse, query, queue_copy = pl.pallas_call(
        functools.partial(lse_kernel, images=images),
        out_shape=(
            pltpu.VMEM((extra, LANES), F32),
            pltpu.VMEM((count, kd), BF16),
            jax.ShapeDtypeStruct(queue.shape, BF16),
        ),
        in_specs=[whole, hbm],
        out_specs=(whole, whole, hbm),
        scratch_shapes=[
            pltpu.VMEM((extra * LANES, kd), F32),
            pltpu.VMEM(queue.shape, BF16),
            pltpu.SemaphoreType.DMA((2,)),
        ],
        compiler_params=pltpu.CompilerParams(vmem_limit_bytes=4 * 2**20),
        name="lse",
    )(query, far(queue))

    chain = [(k, k + 1) for k in range(sections - 1)]
    ticks = images + HOP * (sections - 1)
    sent, turned, *held, marks, blank, tick = first_tick(
        patches, (ln1_gain, w_qkv[0], w_out[0], ln2_gain, w_fc1[0], w_fc2[0]), rows
    )
    weights = (ln1_gain, held[0], held[1], ln2_gain, held[2], held[3])

    def advance(carry):
        tick, came, sent, marks = carry
        for _ in range(UNROLL):
            coming = lax.ppermute(sent, "section", chain)
            sent, marks, tick = run_tick(tick, turned, came, marks, weights, toks)
            came = coming
        return tick, came, sent, marks

    _, came, sent, marks = lax.while_loop(lambda carry: carry[0][0] < ticks - 1, advance, (tick, blank, sent, marks))

    height = -(-(kd // LANES * images + 3 * extra) // 8) * 8
    message = pl.pallas_call(
        functools.partial(head_kernel, toks=toks),
        out_shape=jax.ShapeDtypeStruct((peers, height, LANES), BF16),
        in_specs=[whole] * 11,
        out_specs=whole,
        scratch_shapes=[
            pltpu.VMEM((images, width), F32),
            pltpu.VMEM((rows, width), BF16),
            pltpu.VMEM((rows, 3 * width), BF16),
        ],
        compiler_params=pltpu.CompilerParams(vmem_limit_bytes=12 * 2**20),
        name="head",
    )(hold(came), hold(marks), *held_weights(weights), final_norm_gain.reshape(1, width), w_head, hold(lse))
    got = lax.all_to_all(message, ("dp", "section"), 0, 0, tiled=True)

    keys, loss, total, new_queue = pl.pallas_call(
        functools.partial(final_kernel, images=images, extra=extra, kd=kd),
        out_shape=(
            jax.ShapeDtypeStruct((images, kd), BF16),
            jax.ShapeDtypeStruct((1, images), F32),
            jax.ShapeDtypeStruct((1, 1), F32),
            jax.ShapeDtypeStruct(queue.shape, BF16),
        ),
        in_specs=[smem, whole, whole, whole, hbm],
        out_specs=(whole, whole, whole, hbm),
        scratch_shapes=[pltpu.VMEM((32, kd), BF16), pltpu.SemaphoreType.DMA],
        input_output_aliases={4: 3},
        name="final",
    )(pointer, got, hold(query), owner.reshape(1, count), far(queue_copy))
    return keys, loss.reshape(images), total.reshape(()), new_queue


def solution(mesh):
    placed = (
        P("dp", None, None),
        P("section", None),
        P("section", None, None),
        P("section", None, None),
        P("section", None),
        P("section", None, None),
        P("section", None, None),
        P(),
        P(),
        P("dp", None),
        P(("dp", "section"), None),
        P(),
        P("dp"),
    )
    return jax.shard_map(
        on_device,
        mesh=mesh,
        in_specs=placed,
        out_specs=(P("dp", None), P("dp"), P(), P(("dp", "section"), None)),
        check_vma=False,
    )
```

```python
import functools
import math

import jax
import jax.numpy as jnp
from jax import lax
from jax.experimental import pallas as pl
from jax.experimental.pallas import tpu as pltpu
from jax.sharding import PartitionSpec as P

F32 = jnp.float32
BF16 = jnp.bfloat16
HEAD_DIM = 64
LANES = 128
WIDE = 256
SHARPNESS = 0.2
HOP = 2


def layer_norm(values, gain):
    center = values - jnp.mean(values, axis=-1, keepdims=True)
    spread = jnp.mean(center * center, axis=-1, keepdims=True)
    return center * lax.rsqrt(spread + 1e-06) * gain


def mm(left, right):
    return jnp.dot(left, right, preferred_element_type=F32)


def mm_t(left, right):
    return lax.dot_general(left, right, (((1,), (1,)), ((), ())), preferred_element_type=F32)


def attention_tools(rows, toks):
    pair = LANES // HEAD_DIM
    lane = lax.broadcasted_iota(jnp.int32, (rows, LANES), 1) // HEAD_DIM
    keep = lax.broadcasted_iota(jnp.int32, (rows, rows), 1) < toks
    return pair, lane, keep


def encode(wqkv, wout, g2, wfc1, wfc2, out_ref, norm, qkv, ctx, res, act, toks, ready=None):
    rows, width = norm.shape
    ff = wfc1.shape[1]
    quad = WIDE // HEAD_DIM
    pair, lane, keep = attention_tools(rows, toks)
    scale = 1.0 / math.sqrt(HEAD_DIM)
    ready = ready or (lambda k: None)

    def project(j):
        for part in range(3):
            o = part * width + j * WIDE
            y = mm(norm[...], wqkv[:, o : o + WIDE])
            if part == 0:
                y = y * scale
            qkv[:, o : o + WIDE] = y.astype(BF16)

    def scores(j):
        found = []
        for h in range(quad):
            o = j * WIDE + (h // pair) * LANES
            q = qkv[:, o : o + LANES]
            q = jnp.where(lane == h % pair, q, jnp.zeros_like(q))
            found.append(mm_t(q, qkv[:, width + o : width + o + LANES]))
        return found

    def soften(found):
        out = []
        for s in found:
            s = jnp.where(keep, s, -1e30)
            out.append(jnp.exp(s - jnp.max(s, axis=-1, keepdims=True)).astype(BF16))
        return out

    def mix(j, weights):
        ones = jnp.ones((rows, LANES), BF16)
        for half in range(quad // pair):
            o = j * WIDE + half * LANES
            v = jnp.concatenate([qkv[:, 2 * width + o : 2 * width + o + LANES], ones], axis=1)
            got = None
            for i in range(pair):
                y = mm(weights[half * pair + i], v)
                y = y[:, :LANES] / y[:, LANES:]
                got = y if got is None else jnp.where(lane == i, y, got)
            ctx[:, o : o + LANES] = got.astype(BF16)

    groups = width // WIDE
    late = (groups - 1) * WIDE
    ready(0)
    project(0)
    if groups > 1:
        project(1)
    found = scores(0)
    for j in range(groups):
        coming = None
        if j + 1 < groups:
            coming = scores(j + 1)
        if j + 2 < groups:
            project(j + 2)
        if j + 1 == groups:
            ready(1)
            for n in range(0, width, WIDE):
                res[:, n : n + WIDE] += mm(ctx[:, 0:late], wout[0:late, n : n + WIDE])
        mix(j, soften(found))
        found = coming
    for n in range(0, width, WIDE):
        res[:, n : n + WIDE] += mm(ctx[:, late:width], wout[late:width, n : n + WIDE])
    norm[...] = layer_norm(res[...], g2[...]).astype(BF16)
    ready(2)
    for n in range(0, ff, WIDE):
        t = mm(norm[...], wfc1[:, n : n + WIDE])
        t = 0.5 * t * (1.0 + lax.erf(t * (1.0 / math.sqrt(2.0))))
        act[:, n : n + WIDE] = t.astype(BF16)
    ready(3)
    for n in range(0, width, WIDE):
        out_ref[:, n : n + WIDE] = (res[:, n : n + WIDE] + mm(act[...], wfc2[:, n : n + WIDE])).astype(BF16)


def by_columns(left, right, start, stop, store, compact):
    size = 2 * WIDE if compact else WIDE

    def part(o):
        store(o - start, mm(left, right[:, pl.ds(o, size)]))

    if compact:
        lax.fori_loop(start // size, stop // size, lambda k, _: (part(pl.multiple_of(k * size, size)), 0)[1], 0)
    else:
        for o in range(start, stop, size):
            part(o)


def encode_class(x_ref, g1, wqkv, wout, g2, wfc1, wfc2, norm, qkv, row, toks, compact):
    rows, width = norm.shape
    ff = wfc1.shape[1]
    heads = width // HEAD_DIM
    scale = 1.0 / math.sqrt(HEAD_DIM)
    norm[...] = layer_norm(x_ref[...].astype(F32), g1[...]).astype(BF16)

    def keep(o, y):
        row[:, pl.ds(o, y.shape[1])] = y

    by_columns(norm[0:8, :], wqkv, 0, width, keep, compact)
    q = row[0:1, 0:width] * scale
    own = lax.broadcasted_iota(jnp.int32, (heads, width), 1) // HEAD_DIM
    own = own == lax.broadcasted_iota(jnp.int32, (heads, width), 0)
    q = jnp.where(own, jnp.broadcast_to(q, (heads, width)), 0.0).astype(BF16)

    def keys(o, y):
        qkv[:, pl.ds(o, y.shape[1])] = y.astype(BF16)

    by_columns(norm[...], wqkv, width, 2 * width, keys, compact)
    s = mm_t(q, qkv[:, 0:width])
    s = jnp.where(lax.broadcasted_iota(jnp.int32, s.shape, 1) < toks, s, -1e30)
    e = jnp.exp(s - jnp.max(s, axis=-1, keepdims=True))
    p = (e / jnp.sum(e, axis=-1, keepdims=True)).astype(BF16)
    mixed = mm(p, norm[...]).astype(BF16)

    def values(o, y):
        lane = lax.broadcasted_iota(jnp.int32, y.shape, 1) + o
        mine = lane // HEAD_DIM == lax.broadcasted_iota(jnp.int32, y.shape, 0)
        y = jnp.sum(jnp.where(mine, y, 0.0), axis=0, keepdims=True)
        row[:, pl.ds(o, y.shape[1])] = jnp.broadcast_to(y, (8, y.shape[1]))

    by_columns(mixed, wqkv, 2 * width, 3 * width, values, compact)
    c = row[:, 0:width].astype(BF16)
    by_columns(c, wout, 0, width, keep, compact)
    r = x_ref[0:8, :].astype(F32) + row[:, 0:width]
    n = layer_norm(r, g2[...]).astype(BF16)

    def active(o, t):
        row[:, pl.ds(o, t.shape[1])] = 0.5 * t * (1.0 + lax.erf(t * (1.0 / math.sqrt(2.0))))

    by_columns(n, wfc1, 0, ff, active, compact)
    t = row[:, 0:ff].astype(BF16)
    by_columns(t, wfc2, 0, width, keep, compact)
    return (r + row[:, 0:width])[0:1, :].astype(BF16).astype(F32)


def first_kernel(
    patch_hbm, wqkv_hbm, wout_hbm, wfc1_hbm, wfc2_hbm, g1, g2,
    out_ref, turned, wqkv, wout, wfc1, wfc2, marks, blank, count,
    flat, norm, qkv, ctx, res, act, sems, *, images, toks,
):
    copies = [
        pltpu.make_async_copy(a, b, sems.at[k])
        for k, (a, b) in enumerate(((wqkv_hbm, wqkv), (wout_hbm, wout), (wfc1_hbm, wfc1), (wfc2_hbm, wfc2)))
    ]
    total = toks * images
    fetch = pltpu.make_async_copy(patch_hbm, flat.at[0:total, :], sems.at[4])
    section = lax.axis_index("section")
    pl.when(section == 0)(fetch.start)
    for c in copies:
        c.start()
    marks[...] = jnp.zeros_like(marks)
    blank[...] = jnp.zeros_like(blank)
    count[0] = 1

    @pl.when(section == 0)
    def _():
        span = flat.shape[0]
        flat[total:span, :] = jnp.zeros((span - total, flat.shape[1]), BF16)
        fetch.wait()
        take = WIDE // images
        r = lax.broadcasted_iota(jnp.int32, (WIDE, WIDE), 0)
        c = lax.broadcasted_iota(jnp.int32, (WIDE, WIDE), 1)
        order = (c == (r % take) * images + r // take).astype(F32).astype(BF16)
        rows = turned.shape[1]
        for k in range(0, rows, take):
            got = mm(order, flat[k * images : k * images + WIDE, :]).astype(BF16)
            size = min(take, rows - k)
            for i in range(images):
                turned[i, k : k + size, :] = got[i * take : i * take + size, :]
        x = turned[0].astype(F32)
        res[...] = x
        norm[...] = layer_norm(x, g1[...]).astype(BF16)
        encode(wqkv, wout, g2, wfc1, wfc2, out_ref, norm, qkv, ctx, res, act, toks, ready=lambda k: copies[k].wait())

    @pl.when(section != 0)
    def _():
        for c in copies:
            c.wait()


def first_tick(patches, weights, rows):
    images, toks, width = patches.shape
    g1, wqkv, wout, g2, wfc1, wfc2 = weights
    ff = wfc1.shape[1]
    whole = pl.BlockSpec(memory_space=pltpu.VMEM)
    hbm = pl.BlockSpec(memory_space=pl.ANY)
    span = -(-rows * images // WIDE) * WIDE
    return pl.pallas_call(
        functools.partial(first_kernel, images=images, toks=toks),
        out_shape=(
            pltpu.VMEM((rows, width), BF16),
            pltpu.VMEM((images, rows, width), BF16),
            pltpu.VMEM(wqkv.shape, BF16),
            pltpu.VMEM(wout.shape, BF16),
            pltpu.VMEM(wfc1.shape, BF16),
            pltpu.VMEM(wfc2.shape, BF16),
            pltpu.VMEM((images, width), F32),
            pltpu.VMEM((rows, width), BF16),
            pltpu.SMEM((1,), jnp.int32),
        ),
        in_specs=[hbm] * 5 + [whole] * 2,
        out_specs=(whole,) * 8 + (pl.BlockSpec(memory_space=pltpu.SMEM),),
        scratch_shapes=[
            pltpu.VMEM((span, width), BF16),
            pltpu.VMEM((rows, width), BF16),
            pltpu.VMEM((rows, 3 * width), BF16),
            pltpu.VMEM((rows, width), BF16),
            pltpu.VMEM((rows, width), F32),
            pltpu.VMEM((rows, ff), BF16),
            pltpu.SemaphoreType.DMA((5,)),
        ],
        compiler_params=pltpu.CompilerParams(vmem_limit_bytes=14 * 2**20),
        name="first",
    )(far(patches.transpose(1, 0, 2).reshape(toks * images, width)), far(wqkv), far(wout), far(wfc1), far(wfc2), g1, g2)


def tick_kernel(
    tick, turned, came, marks_in, g1, wqkv, wout, g2, wfc1, wfc2, out_ref, marks, after, norm, qkv, ctx, res, act, row, *, toks
):
    after[0] = tick[0] + 1
    section = lax.axis_index("section")
    last = lax.axis_size("section") - 1
    images = turned.shape[0]
    step = tick[0] - HOP * section
    active = jnp.logical_and(step >= 0, step < images)

    def start(x):
        res[...] = x
        norm[...] = layer_norm(x, g1[...]).astype(BF16)

    @pl.when(jnp.logical_and(active, section != last))
    def _():
        @pl.when(section == 0)
        def _():
            start(turned[step].astype(F32))

        @pl.when(section != 0)
        def _():
            start(came[...].astype(F32))

        encode(wqkv, wout, g2, wfc1, wfc2, out_ref, norm, qkv, ctx, res, act, toks)

    @pl.when(jnp.logical_and(active, section == last))
    def _():
        marks[pl.ds(step, 1), :] = encode_class(came, g1, wqkv, wout, g2, wfc1, wfc2, norm, qkv, row, toks, True)


def hold(x):
    return pltpu.with_memory_space_constraint(x, pltpu.VMEM)


def far(x):
    return pltpu.with_memory_space_constraint(x, pltpu.HBM)


def held_weights(weights):
    g1, wqkv, wout, g2, wfc1, wfc2 = weights
    return g1, hold(wqkv), hold(wout), g2, hold(wfc1), hold(wfc2)


def run_tick(tick, turned, came, marks, weights, toks):
    rows, width = came.shape
    ff = weights[4].shape[1]
    whole = pl.BlockSpec(memory_space=pltpu.VMEM)
    return pl.pallas_call(
        functools.partial(tick_kernel, toks=toks),
        out_shape=(pltpu.VMEM((rows, width), BF16), pltpu.VMEM(marks.shape, F32), pltpu.SMEM((1,), jnp.int32)),
        in_specs=[pl.BlockSpec(memory_space=pltpu.SMEM)] + [whole] * 9,
        out_specs=(whole, whole, pl.BlockSpec(memory_space=pltpu.SMEM)),
        scratch_shapes=[
            pltpu.VMEM((rows, width), BF16),
            pltpu.VMEM((rows, 3 * width), BF16),
            pltpu.VMEM((rows, width), BF16),
            pltpu.VMEM((rows, width), F32),
            pltpu.VMEM((rows, ff), BF16),
            pltpu.VMEM((8, max(ff, width)), F32),
        ],
        input_output_aliases={3: 1},
        compiler_params=pltpu.CompilerParams(vmem_limit_bytes=12 * 2**20),
        name="block",
    )(tick, hold(turned), hold(came), hold(marks), *held_weights(weights))


def merge_kernel(left, right, out_ref):
    half = left.shape[0]
    out_ref[0:half, :] = left[...]
    out_ref[half : 2 * half, :] = right[...]


def merge(left, right):
    whole = pl.BlockSpec(memory_space=pltpu.VMEM)
    return pl.pallas_call(
        merge_kernel,
        out_shape=pltpu.VMEM((2 * left.shape[0], left.shape[1]), left.dtype),
        in_specs=[whole, whole],
        out_specs=whole,
        compiler_params=pltpu.CompilerParams(vmem_limit_bytes=2**20),
        name="merge",
    )(left, right)


def class_kernel(came, marks_in, g1, wqkv, wout, g2, wfc1, wfc2, marks, norm, qkv, row, *, toks):
    step = marks.shape[0] - 2

    @pl.when(lax.axis_index("section") == lax.axis_size("section") - 1)
    def _():
        marks[step : step + 1, :] = encode_class(came, g1, wqkv, wout, g2, wfc1, wfc2, norm, qkv, row, toks, True)


def run_class(came, marks, weights, toks):
    rows, width = came.shape
    whole = pl.BlockSpec(memory_space=pltpu.VMEM)
    return pl.pallas_call(
        functools.partial(class_kernel, toks=toks),
        out_shape=pltpu.VMEM(marks.shape, F32),
        in_specs=[whole] * 8,
        out_specs=whole,
        scratch_shapes=[
            pltpu.VMEM((rows, width), BF16),
            pltpu.VMEM((rows, width), BF16),
            pltpu.VMEM((8, max(weights[4].shape[1], width)), F32),
        ],
        input_output_aliases={1: 0},
        compiler_params=pltpu.CompilerParams(vmem_limit_bytes=12 * 2**20),
        name="class",
    )(hold(came), hold(marks), *held_weights(weights))


def straighten(swapped, ordered, images):
    group = lax.axis_index("dp")
    ordered[...] = jnp.zeros_like(ordered)
    for b in range(swapped.shape[0] // images):
        place = pl.multiple_of(jnp.bitwise_xor(group, b) * images, images)
        ordered[pl.ds(place, images), :] = swapped[b * images : (b + 1) * images, :].astype(F32)


def score_shard(fetch, back, out_ref, ordered, queue):
    lanes = out_ref.shape[1]
    fetch.wait()
    back.start()
    for k in range(out_ref.shape[0]):
        s = mm_t(queue[...], ordered[k * lanes : (k + 1) * lanes, :].astype(BF16)) * (1.0 / SHARPNESS)
        peak = jnp.max(s, axis=0, keepdims=True)
        out_ref[k : k + 1, :] = peak + jnp.log(jnp.sum(jnp.exp(s - peak), axis=0, keepdims=True))
    back.wait()


def early_kernel(swapped, queue_hbm, out_ref, copy_ref, query_ref, ordered, queue, sems, *, images):
    straighten(swapped, ordered, images)
    query_ref[...] = ordered[0 : query_ref.shape[0], :].astype(BF16)

    @pl.when(lax.axis_index("section") == lax.axis_size("section") - 1)
    def _():
        fetch = pltpu.make_async_copy(queue_hbm, queue, sems.at[0])
        back = pltpu.make_async_copy(queue, copy_ref, sems.at[1])
        fetch.start()
        score_shard(fetch, back, out_ref, ordered, queue)


def late_kernel(query, queue_hbm, lse_in, copy_in, out_ref, copy_ref, ordered, queue, sems):
    @pl.when(lax.axis_index("section") != lax.axis_size("section") - 1)
    def _():
        fetch = pltpu.make_async_copy(queue_hbm, queue, sems.at[0])
        back = pltpu.make_async_copy(queue, copy_ref, sems.at[1])
        fetch.start()
        ordered[...] = jnp.zeros_like(ordered)
        ordered[0 : query.shape[0], :] = query[...].astype(F32)
        score_shard(fetch, back, out_ref, ordered, queue)

    @pl.when(lax.axis_index("section") == lax.axis_size("section") - 1)
    def _():
        out_ref[...] = lse_in[...]


def head_kernel(came, marks, g1, wqkv, wout, g2, wfc1, wfc2, gain, head, lse, out_ref, found, norm, qkv, row, *, toks):
    images = found.shape[0]

    @pl.when(lax.axis_index("section") == lax.axis_size("section") - 1)
    def _():
        found[...] = marks[...]
        found[images - 1 : images, :] = encode_class(came, g1, wqkv, wout, g2, wfc1, wfc2, norm, qkv, row, toks, False)

    @pl.when(lax.axis_index("section") != lax.axis_size("section") - 1)
    def _():
        found[...] = jnp.zeros_like(found)

    normed = layer_norm(found[...], gain[...]).astype(BF16)
    z = mm(normed, head[...])
    z = z * lax.rsqrt(1.0 + jnp.sum(z * z, axis=1, keepdims=True))
    kd = z.shape[1]
    peers, rows, lanes = out_ref.shape
    parts = [z[:, o : o + lanes] for o in range(0, kd, lanes)]
    high = lse[...].astype(BF16).astype(F32)
    mid = (lse[...] - high).astype(BF16).astype(F32)
    low = lse[...] - high - mid
    parts += [high, mid, low]
    used = sum(p.shape[0] for p in parts)
    if rows > used:
        parts.append(jnp.zeros((rows - used, lanes), F32))
    block = jnp.concatenate(parts, axis=0).astype(BF16)
    out_ref[...] = jnp.broadcast_to(block[None], out_ref.shape)


def final_kernel(
    pointer, got, query, owner, queue_in, keys_ref, loss_ref, total_ref, queue_ref, window, sem, *, images, extra, kd
):
    section = lax.axis_index("section")
    group = lax.axis_index("dp")
    start = pointer[0]
    share = queue_ref.shape[0]
    local = start - section * share
    span = window.shape[0]
    base = jnp.clip((local // 16) * 16, 0, share - span)
    base = pl.multiple_of(base, 16)
    fetch = pltpu.make_async_copy(queue_ref.at[pl.ds(base, span), :], window, sem)
    fetch.start()
    peers, rows, lanes = got.shape
    halves = kd // lanes
    last = peers // query.shape[0] * images
    count = query.shape[0]
    n_sec = peers * images // count
    pieces = []
    for g in range(count // images):
        src = g * n_sec + n_sec - 1
        one = got[src].astype(F32)
        pieces.append(jnp.concatenate([one[h * images : (h + 1) * images] for h in range(halves)], axis=1))
    keys = jnp.concatenate(pieces, axis=0)
    keys16 = keys.astype(BF16)
    row = lax.broadcasted_iota(jnp.int32, (span, count), 0) + (base - local)
    slot = owner[...] - group * images
    pick = jnp.logical_and(row == slot, jnp.logical_and(slot >= 0, slot < images))
    fresh = mm(pick.astype(F32).astype(BF16), keys16)
    hit = jnp.sum(pick.astype(F32), axis=1, keepdims=True) > 0.5
    fetch.wait()
    window[...] = jnp.where(hit, fresh, window[...].astype(F32)).astype(BF16)
    back = pltpu.make_async_copy(window, queue_ref.at[pl.ds(base, span), :], sem)
    back.start()
    msgs = got[...].astype(F32)
    off = halves * images
    lse = msgs[:, off : off + extra, :] + msgs[:, off + extra : off + 2 * extra, :] + msgs[:, off + 2 * extra : off + 3 * extra, :]
    peak = jnp.max(lse, axis=0)
    negative = peak + jnp.log(jnp.sum(jnp.exp(lse - peak[None]), axis=0))
    square = mm_t(query[...], keys16)
    r = lax.broadcasted_iota(jnp.int32, square.shape, 0)
    c = lax.broadcasted_iota(jnp.int32, square.shape, 1)
    positive = jnp.sum(jnp.where(r == c, square, 0.0), axis=0, keepdims=True) * (1.0 / SHARPNESS)
    positive = jnp.pad(positive, ((0, 0), (0, lanes - count)))
    larger = jnp.maximum(negative, positive)
    loss = larger + jnp.log(jnp.exp(negative - larger) + jnp.exp(positive - larger)) - positive
    lane = lax.broadcasted_iota(jnp.int32, loss.shape, 1)
    total_ref[...] = jnp.sum(jnp.where(lane < count, loss, 0.0), axis=1, keepdims=True) * (1.0 / count)
    turned = pltpu.roll(jnp.broadcast_to(loss, (8, lanes)), lanes - group * images, 1)
    loss_ref[...] = turned[0:1, 0:images]
    mine = got[group * n_sec + n_sec - 1].astype(F32)
    keys_ref[...] = jnp.concatenate([mine[h * images : (h + 1) * images] for h in range(halves)], axis=1).astype(BF16)
    back.wait()


def on_device(
    patches,
    ln1_gain,
    w_qkv,
    w_out,
    ln2_gain,
    w_fc1,
    w_fc2,
    final_norm_gain,
    w_head,
    online_embeddings,
    queue,
    owner,
    pointer,
):
    sections = lax.axis_size("section")
    groups = lax.axis_size("dp")
    section = lax.axis_index("section").astype(jnp.int32)
    group = lax.axis_index("dp").astype(jnp.int32)
    images, toks, width = patches.shape
    kd = w_head.shape[1]
    peers = sections * groups
    count = groups * images
    rows = -(-toks // 8) * 8
    whole = pl.BlockSpec(memory_space=pltpu.VMEM)
    smem = pl.BlockSpec(memory_space=pltpu.SMEM)
    hbm = pl.BlockSpec(memory_space=pl.ANY)

    extra = -(-count // LANES)
    limit = pltpu.CompilerParams(vmem_limit_bytes=4 * 2**20)
    shapes = (pltpu.VMEM((extra, LANES), F32), jax.ShapeDtypeStruct(queue.shape, BF16))
    work = [
        pltpu.VMEM((extra * LANES, kd), F32),
        pltpu.VMEM(queue.shape, BF16),
        pltpu.SemaphoreType.DMA((2,)),
    ]
    chain = [(k, k + 1) for k in range(sections - 1)]
    ticks = images + HOP * (sections - 1)
    hops = [1 << k for k in range(max(groups - 1, 1).bit_length()) if 1 << k < groups]

    def exchange(rows, hop):
        pairs = [(k * sections + j, (k ^ hop) * sections + j) for k in range(groups) for j in range(sections)]
        return lax.ppermute(rows, ("dp", "section"), pairs)

    swapped = online_embeddings
    other = exchange(swapped, hops[0])
    sent, turned, *held, marks, blank, tick = first_tick(
        patches, (ln1_gain, w_qkv[0], w_out[0], ln2_gain, w_fc1[0], w_fc2[0]), rows
    )
    weights = (ln1_gain, held[0], held[1], ln2_gain, held[2], held[3])
    loops = ticks - 4
    unroll = next(k for k in (2, 1) if loops % k == 0)

    def one(tick, came, sent, marks):
        coming = lax.ppermute(sent, "section", chain)
        sent, marks, tick = run_tick(tick, turned, came, marks, weights, toks)
        return tick, coming, sent, marks

    def advance(carry):
        for _ in range(unroll):
            carry = one(*carry)
        return carry

    other, sent = lax.optimization_barrier((other, sent))
    swapped = merge(swapped, other)
    if len(hops) > 1:
        other = exchange(swapped, hops[1])
    tick, came, sent, marks = one(tick, blank, sent, marks)
    for hop in hops[1:]:
        if hop != hops[1]:
            other = exchange(swapped, hop)
        other, sent = lax.optimization_barrier((other, sent))
        swapped = merge(swapped, other)
    lse, queue_copy, query = pl.pallas_call(
        functools.partial(early_kernel, images=images),
        out_shape=shapes + (pltpu.VMEM((count, kd), BF16),),
        in_specs=[whole, hbm],
        out_specs=(whole, hbm, whole),
        scratch_shapes=work,
        compiler_params=limit,
        name="early",
    )(hold(swapped), far(queue))
    lse, sent = lax.optimization_barrier((lse, sent))
    carry = lax.while_loop(lambda carry: carry[0][0] <= loops + 1, advance, (tick, came, sent, marks))
    _, came, sent, marks = carry
    coming = lax.ppermute(sent, "section", chain[-1:])
    marks = run_class(came, marks, weights, toks)
    came = coming

    lse, marks = lax.optimization_barrier((lse, marks))
    lse, queue_copy = pl.pallas_call(
        late_kernel,
        out_shape=shapes,
        in_specs=[whole, hbm, whole, hbm],
        out_specs=(whole, hbm),
        scratch_shapes=work,
        input_output_aliases={3: 1},
        compiler_params=limit,
        name="late",
    )(hold(query), far(queue), hold(lse), far(queue_copy))
    height = -(-(kd // LANES * images + 3 * extra) // 8) * 8
    message = pl.pallas_call(
        functools.partial(head_kernel, toks=toks),
        out_shape=jax.ShapeDtypeStruct((peers, height, LANES), BF16),
        in_specs=[whole] * 11,
        out_specs=whole,
        scratch_shapes=[
            pltpu.VMEM((images, width), F32),
            pltpu.VMEM((rows, width), BF16),
            pltpu.VMEM((rows, 3 * width), BF16),
            pltpu.VMEM((8, max(w_fc1.shape[2], width)), F32),
        ],
        compiler_params=pltpu.CompilerParams(vmem_limit_bytes=12 * 2**20),
        name="head",
    )(hold(came), hold(marks), *held_weights(weights), final_norm_gain.reshape(1, width), w_head, hold(lse))
    got = lax.all_to_all(message, ("dp", "section"), 0, 0, tiled=True)

    keys, loss, total, new_queue = pl.pallas_call(
        functools.partial(final_kernel, images=images, extra=extra, kd=kd),
        out_shape=(
            jax.ShapeDtypeStruct((images, kd), BF16),
            jax.ShapeDtypeStruct((1, images), F32),
            jax.ShapeDtypeStruct((1, 1), F32),
            jax.ShapeDtypeStruct(queue.shape, BF16),
        ),
        in_specs=[smem, whole, whole, whole, hbm],
        out_specs=(whole, whole, whole, hbm),
        scratch_shapes=[pltpu.VMEM((32, kd), BF16), pltpu.SemaphoreType.DMA],
        input_output_aliases={4: 3},
        name="final",
    )(pointer, hold(got), hold(query), owner.reshape(1, count), far(queue_copy))
    return keys, loss.reshape(images), total.reshape(()), new_queue


def solution(mesh):
    placed = (
        P("dp", None, None),
        P("section", None),
        P("section", None, None),
        P("section", None, None),
        P("section", None),
        P("section", None, None),
        P("section", None, None),
        P(),
        P(),
        P("dp", None),
        P(("dp", "section"), None),
        P(),
        P("dp"),
    )
    return jax.shard_map(
        on_device,
        mesh=mesh,
        in_specs=placed,
        out_specs=(P("dp", None), P("dp"), P(), P(("dp", "section"), None)),
        check_vma=False,
    )
```

```python
import functools
import math

import jax
import jax.numpy as jnp
from jax import lax
from jax.experimental import pallas as pl
from jax.experimental.pallas import tpu as pltpu
from jax.sharding import PartitionSpec as P

F32 = jnp.float32
BF16 = jnp.bfloat16
HEAD_DIM = 64
LANES = 128
WIDE = 256
SHARPNESS = 0.2
HOP = 2


def layer_norm(values, gain):
    center = values - jnp.mean(values, axis=-1, keepdims=True)
    spread = jnp.mean(center * center, axis=-1, keepdims=True)
    return center * lax.rsqrt(spread + 1e-06) * gain


def mm(left, right):
    return jnp.dot(left, right, preferred_element_type=F32)


def mm_t(left, right):
    return lax.dot_general(left, right, (((1,), (1,)), ((), ())), preferred_element_type=F32)


def attention_tools(rows, toks):
    pair = LANES // HEAD_DIM
    lane = lax.broadcasted_iota(jnp.int32, (rows, LANES), 1) // HEAD_DIM
    keep = lax.broadcasted_iota(jnp.int32, (rows, rows), 1) < toks
    return pair, lane, keep


def encode(wqkv, wout, g2, wfc1, wfc2, out_ref, norm, qkv, ctx, res, act, toks, ready=None):
    rows, width = norm.shape
    ff = wfc1.shape[1]
    quad = WIDE // HEAD_DIM
    pair, lane, keep = attention_tools(rows, toks)
    scale = 1.0 / math.sqrt(HEAD_DIM)
    ready = ready or (lambda k: None)

    def project(j):
        for part in range(3):
            o = part * width + j * WIDE
            y = mm(norm[...], wqkv[:, o : o + WIDE])
            if part == 0:
                y = y * scale
            qkv[:, o : o + WIDE] = y.astype(BF16)

    def scores(j):
        found = []
        for h in range(quad):
            o = j * WIDE + (h // pair) * LANES
            q = qkv[:, o : o + LANES]
            q = jnp.where(lane == h % pair, q, jnp.zeros_like(q))
            found.append(mm_t(q, qkv[:, width + o : width + o + LANES]))
        return found

    def soften(found):
        out = []
        for s in found:
            s = jnp.where(keep, s, -1e30)
            out.append(jnp.exp(s - jnp.max(s, axis=-1, keepdims=True)).astype(BF16))
        return out

    def mix(j, weights):
        ones = jnp.ones((rows, LANES), BF16)
        for half in range(quad // pair):
            o = j * WIDE + half * LANES
            v = jnp.concatenate([qkv[:, 2 * width + o : 2 * width + o + LANES], ones], axis=1)
            got = None
            for i in range(pair):
                y = mm(weights[half * pair + i], v)
                y = y[:, :LANES] / y[:, LANES:]
                got = y if got is None else jnp.where(lane == i, y, got)
            ctx[:, o : o + LANES] = got.astype(BF16)

    groups = width // WIDE
    late = (groups - 1) * WIDE
    ready(0)
    project(0)
    if groups > 1:
        project(1)
    found = scores(0)
    for j in range(groups):
        coming = None
        if j + 1 < groups:
            coming = scores(j + 1)
        if j + 2 < groups:
            project(j + 2)
        if j + 1 == groups:
            ready(1)
            for n in range(0, width, WIDE):
                res[:, n : n + WIDE] += mm(ctx[:, 0:late], wout[0:late, n : n + WIDE])
        mix(j, soften(found))
        found = coming
    for n in range(0, width, WIDE):
        res[:, n : n + WIDE] += mm(ctx[:, late:width], wout[late:width, n : n + WIDE])
    norm[...] = layer_norm(res[...], g2[...]).astype(BF16)
    ready(2)
    for n in range(0, ff, WIDE):
        t = mm(norm[...], wfc1[:, n : n + WIDE])
        t = 0.5 * t * (1.0 + lax.erf(t * (1.0 / math.sqrt(2.0))))
        act[:, n : n + WIDE] = t.astype(BF16)
    ready(3)
    for n in range(0, width, WIDE):
        out_ref[:, n : n + WIDE] = (res[:, n : n + WIDE] + mm(act[...], wfc2[:, n : n + WIDE])).astype(BF16)


def by_columns(left, right, start, stop, store, compact):
    size = 2 * WIDE if compact else WIDE

    def part(o):
        store(o - start, mm(left, right[:, pl.ds(o, size)]))

    if compact:
        lax.fori_loop(start // size, stop // size, lambda k, _: (part(pl.multiple_of(k * size, size)), 0)[1], 0)
    else:
        for o in range(start, stop, size):
            part(o)


def encode_class(x_ref, g1, wqkv, wout, g2, wfc1, wfc2, norm, qkv, row, toks, compact):
    rows, width = norm.shape
    ff = wfc1.shape[1]
    heads = width // HEAD_DIM
    scale = 1.0 / math.sqrt(HEAD_DIM)
    norm[...] = layer_norm(x_ref[...].astype(F32), g1[...]).astype(BF16)

    def keep(o, y):
        row[:, pl.ds(o, y.shape[1])] = y

    by_columns(norm[0:8, :], wqkv, 0, width, keep, compact)
    q = row[0:1, 0:width] * scale
    own = lax.broadcasted_iota(jnp.int32, (heads, width), 1) // HEAD_DIM
    own = own == lax.broadcasted_iota(jnp.int32, (heads, width), 0)
    q = jnp.where(own, jnp.broadcast_to(q, (heads, width)), 0.0).astype(BF16)

    def keys(o, y):
        qkv[:, pl.ds(o, y.shape[1])] = y.astype(BF16)

    by_columns(norm[...], wqkv, width, 2 * width, keys, compact)
    s = mm_t(q, qkv[:, 0:width])
    s = jnp.where(lax.broadcasted_iota(jnp.int32, s.shape, 1) < toks, s, -1e30)
    e = jnp.exp(s - jnp.max(s, axis=-1, keepdims=True))
    p = (e / jnp.sum(e, axis=-1, keepdims=True)).astype(BF16)
    mixed = mm(p, norm[...]).astype(BF16)

    def values(o, y):
        lane = lax.broadcasted_iota(jnp.int32, y.shape, 1) + o
        mine = lane // HEAD_DIM == lax.broadcasted_iota(jnp.int32, y.shape, 0)
        y = jnp.sum(jnp.where(mine, y, 0.0), axis=0, keepdims=True)
        row[:, pl.ds(o, y.shape[1])] = jnp.broadcast_to(y, (8, y.shape[1]))

    by_columns(mixed, wqkv, 2 * width, 3 * width, values, compact)
    c = row[:, 0:width].astype(BF16)
    by_columns(c, wout, 0, width, keep, compact)
    r = x_ref[0:8, :].astype(F32) + row[:, 0:width]
    n = layer_norm(r, g2[...]).astype(BF16)

    def active(o, t):
        row[:, pl.ds(o, t.shape[1])] = 0.5 * t * (1.0 + lax.erf(t * (1.0 / math.sqrt(2.0))))

    by_columns(n, wfc1, 0, ff, active, compact)
    t = row[:, 0:ff].astype(BF16)
    by_columns(t, wfc2, 0, width, keep, compact)
    return (r + row[:, 0:width])[0:1, :].astype(BF16).astype(F32)


def first_kernel(
    patch_hbm, wqkv_hbm, wout_hbm, wfc1_hbm, wfc2_hbm, g1, g2,
    out_ref, turned, wqkv, wout, wfc1, wfc2, marks, blank, count,
    flat, norm, qkv, ctx, res, act, sems, *, images, toks,
):
    copies = [
        pltpu.make_async_copy(a, b, sems.at[k])
        for k, (a, b) in enumerate(((wqkv_hbm, wqkv), (wout_hbm, wout), (wfc1_hbm, wfc1), (wfc2_hbm, wfc2)))
    ]
    total = toks * images
    fetch = pltpu.make_async_copy(patch_hbm, flat.at[0:total, :], sems.at[4])
    section = lax.axis_index("section")
    pl.when(section == 0)(fetch.start)
    for c in copies:
        c.start()
    marks[...] = jnp.zeros_like(marks)
    blank[...] = jnp.zeros_like(blank)
    count[0] = 1

    @pl.when(section == 0)
    def _():
        span = flat.shape[0]
        flat[total:span, :] = jnp.zeros((span - total, flat.shape[1]), BF16)
        fetch.wait()
        take = WIDE // images
        r = lax.broadcasted_iota(jnp.int32, (WIDE, WIDE), 0)
        c = lax.broadcasted_iota(jnp.int32, (WIDE, WIDE), 1)
        order = (c == (r % take) * images + r // take).astype(F32).astype(BF16)
        rows = turned.shape[1]
        for k in range(0, rows, take):
            got = mm(order, flat[k * images : k * images + WIDE, :]).astype(BF16)
            size = min(take, rows - k)
            for i in range(images):
                turned[i, k : k + size, :] = got[i * take : i * take + size, :]
        x = turned[0].astype(F32)
        res[...] = x
        norm[...] = layer_norm(x, g1[...]).astype(BF16)
        encode(wqkv, wout, g2, wfc1, wfc2, out_ref, norm, qkv, ctx, res, act, toks, ready=lambda k: copies[k].wait())

    @pl.when(section != 0)
    def _():
        for c in copies:
            c.wait()


def first_tick(patches, weights, rows):
    images, toks, width = patches.shape
    g1, wqkv, wout, g2, wfc1, wfc2 = weights
    ff = wfc1.shape[1]
    whole = pl.BlockSpec(memory_space=pltpu.VMEM)
    hbm = pl.BlockSpec(memory_space=pl.ANY)
    span = -(-rows * images // WIDE) * WIDE
    return pl.pallas_call(
        functools.partial(first_kernel, images=images, toks=toks),
        out_shape=(
            pltpu.VMEM((rows, width), BF16),
            pltpu.VMEM((images, rows, width), BF16),
            pltpu.VMEM(wqkv.shape, BF16),
            pltpu.VMEM(wout.shape, BF16),
            pltpu.VMEM(wfc1.shape, BF16),
            pltpu.VMEM(wfc2.shape, BF16),
            pltpu.VMEM((images, width), F32),
            pltpu.VMEM((rows, width), BF16),
            pltpu.SMEM((1,), jnp.int32),
        ),
        in_specs=[hbm] * 5 + [whole] * 2,
        out_specs=(whole,) * 8 + (pl.BlockSpec(memory_space=pltpu.SMEM),),
        scratch_shapes=[
            pltpu.VMEM((span, width), BF16),
            pltpu.VMEM((rows, width), BF16),
            pltpu.VMEM((rows, 3 * width), BF16),
            pltpu.VMEM((rows, width), BF16),
            pltpu.VMEM((rows, width), F32),
            pltpu.VMEM((rows, ff), BF16),
            pltpu.SemaphoreType.DMA((5,)),
        ],
        compiler_params=pltpu.CompilerParams(vmem_limit_bytes=14 * 2**20),
        name="first",
    )(far(patches.transpose(1, 0, 2).reshape(toks * images, width)), far(wqkv), far(wout), far(wfc1), far(wfc2), g1, g2)


def tick_kernel(
    tick, turned, came, marks_in, g1, wqkv, wout, g2, wfc1, wfc2, out_ref, marks, after, norm, qkv, ctx, res, act, row, *, toks
):
    after[0] = tick[0] + 1
    section = lax.axis_index("section")
    last = lax.axis_size("section") - 1
    images = turned.shape[0]
    step = tick[0] - HOP * section
    active = jnp.logical_and(step >= 0, step < images)

    def start(x):
        res[...] = x
        norm[...] = layer_norm(x, g1[...]).astype(BF16)

    @pl.when(jnp.logical_and(active, section != last))
    def _():
        @pl.when(section == 0)
        def _():
            start(turned[step].astype(F32))

        @pl.when(section != 0)
        def _():
            start(came[...].astype(F32))

        encode(wqkv, wout, g2, wfc1, wfc2, out_ref, norm, qkv, ctx, res, act, toks)

    @pl.when(jnp.logical_and(active, section == last))
    def _():
        marks[pl.ds(step, 1), :] = encode_class(came, g1, wqkv, wout, g2, wfc1, wfc2, norm, qkv, row, toks, True)


def hold(x):
    return pltpu.with_memory_space_constraint(x, pltpu.VMEM)


def far(x):
    return pltpu.with_memory_space_constraint(x, pltpu.HBM)


def held_weights(weights):
    g1, wqkv, wout, g2, wfc1, wfc2 = weights
    return g1, hold(wqkv), hold(wout), g2, hold(wfc1), hold(wfc2)


def run_tick(tick, turned, came, marks, weights, toks):
    rows, width = came.shape
    ff = weights[4].shape[1]
    whole = pl.BlockSpec(memory_space=pltpu.VMEM)
    return pl.pallas_call(
        functools.partial(tick_kernel, toks=toks),
        out_shape=(pltpu.VMEM((rows, width), BF16), pltpu.VMEM(marks.shape, F32), pltpu.SMEM((1,), jnp.int32)),
        in_specs=[pl.BlockSpec(memory_space=pltpu.SMEM)] + [whole] * 9,
        out_specs=(whole, whole, pl.BlockSpec(memory_space=pltpu.SMEM)),
        scratch_shapes=[
            pltpu.VMEM((rows, width), BF16),
            pltpu.VMEM((rows, 3 * width), BF16),
            pltpu.VMEM((rows, width), BF16),
            pltpu.VMEM((rows, width), F32),
            pltpu.VMEM((rows, ff), BF16),
            pltpu.VMEM((8, max(ff, width)), F32),
        ],
        input_output_aliases={3: 1},
        compiler_params=pltpu.CompilerParams(vmem_limit_bytes=12 * 2**20),
        name="block",
    )(tick, hold(turned), hold(came), hold(marks), *held_weights(weights))


def merge_kernel(left, right, out_ref):
    half = left.shape[0]
    out_ref[0:half, :] = left[...]
    out_ref[half : 2 * half, :] = right[...]


def merge(left, right):
    whole = pl.BlockSpec(memory_space=pltpu.VMEM)
    return pl.pallas_call(
        merge_kernel,
        out_shape=pltpu.VMEM((2 * left.shape[0], left.shape[1]), left.dtype),
        in_specs=[whole, whole],
        out_specs=whole,
        compiler_params=pltpu.CompilerParams(vmem_limit_bytes=2**20),
        name="merge",
    )(left, right)


def class_kernel(came, marks_in, g1, wqkv, wout, g2, wfc1, wfc2, marks, norm, qkv, row, *, toks):
    step = marks.shape[0] - 2

    @pl.when(lax.axis_index("section") == lax.axis_size("section") - 1)
    def _():
        marks[step : step + 1, :] = encode_class(came, g1, wqkv, wout, g2, wfc1, wfc2, norm, qkv, row, toks, True)


def run_class(came, marks, weights, toks):
    rows, width = came.shape
    whole = pl.BlockSpec(memory_space=pltpu.VMEM)
    return pl.pallas_call(
        functools.partial(class_kernel, toks=toks),
        out_shape=pltpu.VMEM(marks.shape, F32),
        in_specs=[whole] * 8,
        out_specs=whole,
        scratch_shapes=[
            pltpu.VMEM((rows, width), BF16),
            pltpu.VMEM((rows, width), BF16),
            pltpu.VMEM((8, max(weights[4].shape[1], width)), F32),
        ],
        input_output_aliases={1: 0},
        compiler_params=pltpu.CompilerParams(vmem_limit_bytes=12 * 2**20),
        name="class",
    )(hold(came), hold(marks), *held_weights(weights))


def straighten(swapped, ordered, images):
    group = lax.axis_index("dp")
    ordered[...] = jnp.zeros_like(ordered)
    for b in range(swapped.shape[0] // images):
        place = pl.multiple_of(jnp.bitwise_xor(group, b) * images, images)
        ordered[pl.ds(place, images), :] = swapped[b * images : (b + 1) * images, :].astype(F32)


def score_shard(fetch, back, out_ref, ordered, queue):
    lanes = out_ref.shape[1]
    fetch.wait()
    back.start()
    for k in range(out_ref.shape[0]):
        s = mm_t(queue[...], ordered[k * lanes : (k + 1) * lanes, :].astype(BF16)) * (1.0 / SHARPNESS)
        peak = jnp.max(s, axis=0, keepdims=True)
        out_ref[k : k + 1, :] = peak + jnp.log(jnp.sum(jnp.exp(s - peak), axis=0, keepdims=True))
    back.wait()


def early_kernel(swapped, queue_hbm, out_ref, copy_ref, query_ref, ordered, queue, sems, *, images):
    straighten(swapped, ordered, images)
    query_ref[...] = ordered[0 : query_ref.shape[0], :].astype(BF16)

    @pl.when(lax.axis_index("section") == lax.axis_size("section") - 1)
    def _():
        fetch = pltpu.make_async_copy(queue_hbm, queue, sems.at[0])
        back = pltpu.make_async_copy(queue, copy_ref, sems.at[1])
        fetch.start()
        score_shard(fetch, back, out_ref, ordered, queue)


def window_base(pointer, share, span):
    local = pointer[0] - lax.axis_index("section") * share
    return local, pl.multiple_of(jnp.clip((local // 16) * 16, 0, share - span), 16)


def late_kernel(
    query, queue_hbm, pointer, owner, lse_in, copy_in,
    out_ref, copy_ref, window, owner_ref, pointer_ref, ordered, queue, sems,
):
    share, span = queue_hbm.shape[0], window.shape[0]
    pointer_ref[0] = pointer[0]
    owner_ref[...] = owner[...]
    _, base = window_base(pointer, share, span)
    bring = pltpu.make_async_copy(queue_hbm.at[pl.ds(base, span), :], window, sems.at[2])
    bring.start()

    @pl.when(lax.axis_index("section") != lax.axis_size("section") - 1)
    def _():
        fetch = pltpu.make_async_copy(queue_hbm, queue, sems.at[0])
        back = pltpu.make_async_copy(queue, copy_ref, sems.at[1])
        fetch.start()
        ordered[...] = jnp.zeros_like(ordered)
        ordered[0 : query.shape[0], :] = query[...].astype(F32)
        score_shard(fetch, back, out_ref, ordered, queue)

    @pl.when(lax.axis_index("section") == lax.axis_size("section") - 1)
    def _():
        out_ref[...] = lse_in[...]

    bring.wait()


def head_kernel(came, marks, g1, wqkv, wout, g2, wfc1, wfc2, gain, head, lse, out_ref, found, norm, qkv, row, *, toks):
    images = found.shape[0]

    @pl.when(lax.axis_index("section") == lax.axis_size("section") - 1)
    def _():
        found[...] = marks[...]
        found[images - 1 : images, :] = encode_class(came, g1, wqkv, wout, g2, wfc1, wfc2, norm, qkv, row, toks, False)

    @pl.when(lax.axis_index("section") != lax.axis_size("section") - 1)
    def _():
        found[...] = jnp.zeros_like(found)

    normed = layer_norm(found[...], gain[...]).astype(BF16)
    z = mm(normed, head[...])
    z = z * lax.rsqrt(1.0 + jnp.sum(z * z, axis=1, keepdims=True))
    kd = z.shape[1]
    peers, rows, lanes = out_ref.shape
    parts = [z[:, o : o + lanes] for o in range(0, kd, lanes)]
    high = lse[...].astype(BF16).astype(F32)
    mid = (lse[...] - high).astype(BF16).astype(F32)
    low = lse[...] - high - mid
    parts += [high, mid, low]
    used = sum(p.shape[0] for p in parts)
    if rows > used:
        parts.append(jnp.zeros((rows - used, lanes), F32))
    block = jnp.concatenate(parts, axis=0).astype(BF16)
    out_ref[...] = jnp.broadcast_to(block[None], out_ref.shape)


def final_kernel(
    pointer, got, query, owner, window, queue_in, keys_ref, loss_ref, total_ref, queue_ref, merged, sem, *, images, kd
):
    section = lax.axis_index("section")
    group = lax.axis_index("dp")
    span = window.shape[0]
    local, base = window_base(pointer, queue_ref.shape[0], span)
    extra = -(-query.shape[0] // got.shape[2])
    peers, rows, lanes = got.shape
    halves = kd // lanes
    count = query.shape[0]
    n_sec = peers * images // count
    pieces = []
    for g in range(count // images):
        src = g * n_sec + n_sec - 1
        one = got[src].astype(F32)
        pieces.append(jnp.concatenate([one[h * images : (h + 1) * images] for h in range(halves)], axis=1))
    keys = jnp.concatenate(pieces, axis=0)
    keys16 = keys.astype(BF16)
    row = lax.broadcasted_iota(jnp.int32, (span, count), 0) + (base - local)
    slot = owner[...] - group * images
    pick = jnp.logical_and(row == slot, jnp.logical_and(slot >= 0, slot < images))
    fresh = mm(pick.astype(F32).astype(BF16), keys16)
    hit = jnp.sum(pick.astype(F32), axis=1, keepdims=True) > 0.5
    merged[...] = jnp.where(hit, fresh, window[...].astype(F32)).astype(BF16)
    back = pltpu.make_async_copy(merged, queue_ref.at[pl.ds(base, span), :], sem)
    back.start()
    msgs = got[...].astype(F32)
    off = halves * images
    lse = msgs[:, off : off + extra, :] + msgs[:, off + extra : off + 2 * extra, :] + msgs[:, off + 2 * extra : off + 3 * extra, :]
    peak = jnp.max(lse, axis=0)
    negative = peak + jnp.log(jnp.sum(jnp.exp(lse - peak[None]), axis=0))
    square = mm_t(query[...], keys16)
    r = lax.broadcasted_iota(jnp.int32, square.shape, 0)
    c = lax.broadcasted_iota(jnp.int32, square.shape, 1)
    positive = jnp.sum(jnp.where(r == c, square, 0.0), axis=0, keepdims=True) * (1.0 / SHARPNESS)
    positive = jnp.pad(positive, ((0, 0), (0, lanes - count)))
    larger = jnp.maximum(negative, positive)
    loss = larger + jnp.log(jnp.exp(negative - larger) + jnp.exp(positive - larger)) - positive
    lane = lax.broadcasted_iota(jnp.int32, loss.shape, 1)
    total_ref[...] = jnp.sum(jnp.where(lane < count, loss, 0.0), axis=1, keepdims=True) * (1.0 / count)
    turned = pltpu.roll(jnp.broadcast_to(loss, (8, lanes)), lanes - group * images, 1)
    loss_ref[...] = turned[0:1, 0:images]
    mine = got[group * n_sec + n_sec - 1].astype(F32)
    keys_ref[...] = jnp.concatenate([mine[h * images : (h + 1) * images] for h in range(halves)], axis=1).astype(BF16)
    back.wait()


def on_device(
    patches,
    ln1_gain,
    w_qkv,
    w_out,
    ln2_gain,
    w_fc1,
    w_fc2,
    final_norm_gain,
    w_head,
    online_embeddings,
    queue,
    owner,
    pointer,
):
    sections = lax.axis_size("section")
    groups = lax.axis_size("dp")
    section = lax.axis_index("section").astype(jnp.int32)
    group = lax.axis_index("dp").astype(jnp.int32)
    images, toks, width = patches.shape
    kd = w_head.shape[1]
    peers = sections * groups
    count = groups * images
    rows = -(-toks // 8) * 8
    whole = pl.BlockSpec(memory_space=pltpu.VMEM)
    smem = pl.BlockSpec(memory_space=pltpu.SMEM)
    hbm = pl.BlockSpec(memory_space=pl.ANY)

    extra = -(-count // LANES)
    limit = pltpu.CompilerParams(vmem_limit_bytes=4 * 2**20)
    shapes = (pltpu.VMEM((extra, LANES), F32), jax.ShapeDtypeStruct(queue.shape, BF16))
    work = [
        pltpu.VMEM((extra * LANES, kd), F32),
        pltpu.VMEM(queue.shape, BF16),
        pltpu.SemaphoreType.DMA((3,)),
    ]
    chain = [(k, k + 1) for k in range(sections - 1)]
    ticks = images + HOP * (sections - 1)
    hops = [1 << k for k in range(max(groups - 1, 1).bit_length()) if 1 << k < groups]

    def exchange(rows, hop):
        pairs = [(k * sections + j, (k ^ hop) * sections + j) for k in range(groups) for j in range(sections)]
        return lax.ppermute(rows, ("dp", "section"), pairs)

    swapped = online_embeddings
    other = exchange(swapped, hops[0])
    sent, turned, *held, marks, blank, tick = first_tick(
        patches, (ln1_gain, w_qkv[0], w_out[0], ln2_gain, w_fc1[0], w_fc2[0]), rows
    )
    weights = (ln1_gain, held[0], held[1], ln2_gain, held[2], held[3])
    loops = ticks - 4
    unroll = next(k for k in (2, 1) if loops % k == 0)

    def one(tick, came, sent, marks):
        coming = lax.ppermute(sent, "section", chain)
        sent, marks, tick = run_tick(tick, turned, came, marks, weights, toks)
        return tick, coming, sent, marks

    def advance(carry):
        for _ in range(unroll):
            carry = one(*carry)
        return carry

    other, sent = lax.optimization_barrier((other, sent))
    swapped = merge(swapped, other)
    if len(hops) > 1:
        other = exchange(swapped, hops[1])
    tick, came, sent, marks = one(tick, blank, sent, marks)
    for hop in hops[1:]:
        if hop != hops[1]:
            other = exchange(swapped, hop)
        other, sent = lax.optimization_barrier((other, sent))
        swapped = merge(swapped, other)
    lse, queue_copy, query = pl.pallas_call(
        functools.partial(early_kernel, images=images),
        out_shape=shapes + (pltpu.VMEM((count, kd), BF16),),
        in_specs=[whole, hbm],
        out_specs=(whole, hbm, whole),
        scratch_shapes=work,
        compiler_params=limit,
        name="early",
    )(hold(swapped), far(queue))
    lse, sent = lax.optimization_barrier((lse, sent))
    carry = lax.while_loop(lambda carry: carry[0][0] <= loops + 1, advance, (tick, came, sent, marks))
    _, came, sent, marks = carry
    coming = lax.ppermute(sent, "section", chain[-1:])
    marks = run_class(came, marks, weights, toks)
    came = coming

    lse, marks = lax.optimization_barrier((lse, marks))
    lse, queue_copy, window, owner_row, start = pl.pallas_call(
        late_kernel,
        out_shape=shapes
        + (
            pltpu.VMEM((32, kd), BF16),
            pltpu.VMEM((1, count), jnp.int32),
            pltpu.SMEM((1,), jnp.int32),
        ),
        in_specs=[whole, hbm, smem, whole, whole, hbm],
        out_specs=(whole, hbm, whole, whole, smem),
        scratch_shapes=work,
        input_output_aliases={5: 1},
        compiler_params=limit,
        name="late",
    )(hold(query), far(queue), pointer, owner.reshape(1, count), hold(lse), far(queue_copy))
    height = -(-(kd // LANES * images + 3 * extra) // 8) * 8
    message = pl.pallas_call(
        functools.partial(head_kernel, toks=toks),
        out_shape=jax.ShapeDtypeStruct((peers, height, LANES), BF16),
        in_specs=[whole] * 11,
        out_specs=whole,
        scratch_shapes=[
            pltpu.VMEM((images, width), F32),
            pltpu.VMEM((rows, width), BF16),
            pltpu.VMEM((rows, 3 * width), BF16),
            pltpu.VMEM((8, max(w_fc1.shape[2], width)), F32),
        ],
        compiler_params=pltpu.CompilerParams(vmem_limit_bytes=12 * 2**20),
        name="head",
    )(hold(came), hold(marks), *held_weights(weights), final_norm_gain.reshape(1, width), w_head, hold(lse))
    got = lax.all_to_all(message, ("dp", "section"), 0, 0, tiled=True)

    keys, loss, total, new_queue = pl.pallas_call(
        functools.partial(final_kernel, images=images, kd=kd),
        out_shape=(
            jax.ShapeDtypeStruct((images, kd), BF16),
            jax.ShapeDtypeStruct((1, images), F32),
            jax.ShapeDtypeStruct((1, 1), F32),
            jax.ShapeDtypeStruct(queue.shape, BF16),
        ),
        in_specs=[smem, whole, whole, whole, whole, hbm],
        out_specs=(whole, whole, whole, hbm),
        scratch_shapes=[pltpu.VMEM((32, kd), BF16), pltpu.SemaphoreType.DMA],
        input_output_aliases={5: 3},
        name="final",
    )(start, hold(got), hold(query), hold(owner_row), hold(window), far(queue_copy))
    return keys, loss.reshape(images), total.reshape(()), new_queue


def solution(mesh):
    placed = (
        P("dp", None, None),
        P("section", None),
        P("section", None, None),
        P("section", None, None),
        P("section", None),
        P("section", None, None),
        P("section", None, None),
        P(),
        P(),
        P("dp", None),
        P(("dp", "section"), None),
        P(),
        P("dp"),
    )
    return jax.shard_map(
        on_device,
        mesh=mesh,
        in_specs=placed,
        out_specs=(P("dp", None), P("dp"), P(), P(("dp", "section"), None)),
        check_vma=False,
    )
```

```python
import functools
import math

import jax
import jax.numpy as jnp
from jax import lax
from jax.experimental import pallas as pl
from jax.experimental.pallas import tpu as pltpu
from jax.sharding import PartitionSpec as P

F32 = jnp.float32
BF16 = jnp.bfloat16
HEAD_DIM = 64
LANES = 128
WIDE = 256
SHARPNESS = 0.2
HOP = 2


def layer_norm(values, gain):
    center = values - jnp.mean(values, axis=-1, keepdims=True)
    spread = jnp.mean(center * center, axis=-1, keepdims=True)
    return center * lax.rsqrt(spread + 1e-06) * gain


def mm(left, right):
    return jnp.dot(left, right, preferred_element_type=F32)


def mm_t(left, right):
    return lax.dot_general(left, right, (((1,), (1,)), ((), ())), preferred_element_type=F32)


def attention_tools(rows, toks):
    pair = LANES // HEAD_DIM
    lane = lax.broadcasted_iota(jnp.int32, (rows, LANES), 1) // HEAD_DIM
    keep = lax.broadcasted_iota(jnp.int32, (rows, rows), 1) < toks
    return pair, lane, keep


def encode(wqkv, wout, g2, wfc1, wfc2, out_ref, norm, qkv, ctx, res, act, toks, ready=None):
    rows, width = norm.shape
    ff = wfc1.shape[1]
    quad = WIDE // HEAD_DIM
    pair, lane, keep = attention_tools(rows, toks)
    scale = 1.0 / math.sqrt(HEAD_DIM)
    ready = ready or (lambda k: None)

    def project(j):
        for part in range(3):
            o = part * width + j * WIDE
            y = mm(norm[...], wqkv[:, o : o + WIDE])
            if part == 0:
                y = y * scale
            qkv[:, o : o + WIDE] = y.astype(BF16)

    def scores(j):
        found = []
        for h in range(quad):
            o = j * WIDE + (h // pair) * LANES
            q = qkv[:, o : o + LANES]
            q = jnp.where(lane == h % pair, q, jnp.zeros_like(q))
            found.append(mm_t(q, qkv[:, width + o : width + o + LANES]))
        return found

    def soften(found):
        out = []
        for s in found:
            s = jnp.where(keep, s, -1e30)
            out.append(jnp.exp(s - jnp.max(s, axis=-1, keepdims=True)).astype(BF16))
        return out

    def mix(j, weights):
        ones = jnp.ones((rows, LANES), BF16)
        for half in range(quad // pair):
            o = j * WIDE + half * LANES
            v = jnp.concatenate([qkv[:, 2 * width + o : 2 * width + o + LANES], ones], axis=1)
            got = None
            for i in range(pair):
                y = mm(weights[half * pair + i], v)
                y = y[:, :LANES] / y[:, LANES:]
                got = y if got is None else jnp.where(lane == i, y, got)
            ctx[:, o : o + LANES] = got.astype(BF16)

    groups = width // WIDE
    late = (groups - 1) * WIDE
    ready(0)
    project(0)
    if groups > 1:
        project(1)
    found = scores(0)
    for j in range(groups):
        coming = None
        if j + 1 < groups:
            coming = scores(j + 1)
        if j + 2 < groups:
            project(j + 2)
        if j + 1 == groups:
            ready(1)
            for n in range(0, width, WIDE):
                res[:, n : n + WIDE] += mm(ctx[:, 0:late], wout[0:late, n : n + WIDE])
        mix(j, soften(found))
        found = coming
    for n in range(0, width, WIDE):
        res[:, n : n + WIDE] += mm(ctx[:, late:width], wout[late:width, n : n + WIDE])
    norm[...] = layer_norm(res[...], g2[...]).astype(BF16)
    ready(2)
    for n in range(0, ff, WIDE):
        t = mm(norm[...], wfc1[:, n : n + WIDE])
        t = 0.5 * t * (1.0 + lax.erf(t * (1.0 / math.sqrt(2.0))))
        act[:, n : n + WIDE] = t.astype(BF16)
    ready(3)
    for n in range(0, width, WIDE):
        out_ref[:, n : n + WIDE] = (res[:, n : n + WIDE] + mm(act[...], wfc2[:, n : n + WIDE])).astype(BF16)


def by_columns(left, right, start, stop, store, compact):
    size = 2 * WIDE if compact else WIDE

    def part(o):
        store(o - start, mm(left, right[:, pl.ds(o, size)]))

    if compact:
        lax.fori_loop(start // size, stop // size, lambda k, _: (part(pl.multiple_of(k * size, size)), 0)[1], 0)
    else:
        for o in range(start, stop, size):
            part(o)


def encode_class(x_ref, g1, wqkv, wout, g2, wfc1, wfc2, norm, qkv, row, toks, compact):
    rows, width = norm.shape
    ff = wfc1.shape[1]
    heads = width // HEAD_DIM
    scale = 1.0 / math.sqrt(HEAD_DIM)
    norm[...] = layer_norm(x_ref[...].astype(F32), g1[...]).astype(BF16)

    def keep(o, y):
        row[:, pl.ds(o, y.shape[1])] = y

    by_columns(norm[0:8, :], wqkv, 0, width, keep, compact)
    q = row[0:1, 0:width] * scale
    own = lax.broadcasted_iota(jnp.int32, (heads, width), 1) // HEAD_DIM
    own = own == lax.broadcasted_iota(jnp.int32, (heads, width), 0)
    q = jnp.where(own, jnp.broadcast_to(q, (heads, width)), 0.0).astype(BF16)

    def keys(o, y):
        qkv[:, pl.ds(o, y.shape[1])] = y.astype(BF16)

    by_columns(norm[...], wqkv, width, 2 * width, keys, compact)
    s = mm_t(q, qkv[:, 0:width])
    s = jnp.where(lax.broadcasted_iota(jnp.int32, s.shape, 1) < toks, s, -1e30)
    e = jnp.exp(s - jnp.max(s, axis=-1, keepdims=True))
    p = (e / jnp.sum(e, axis=-1, keepdims=True)).astype(BF16)
    mixed = mm(p, norm[...]).astype(BF16)

    def values(o, y):
        lane = lax.broadcasted_iota(jnp.int32, y.shape, 1) + o
        mine = lane // HEAD_DIM == lax.broadcasted_iota(jnp.int32, y.shape, 0)
        y = jnp.sum(jnp.where(mine, y, 0.0), axis=0, keepdims=True)
        row[:, pl.ds(o, y.shape[1])] = jnp.broadcast_to(y, (8, y.shape[1]))

    by_columns(mixed, wqkv, 2 * width, 3 * width, values, compact)
    c = row[:, 0:width].astype(BF16)
    by_columns(c, wout, 0, width, keep, compact)
    r = x_ref[0:8, :].astype(F32) + row[:, 0:width]
    n = layer_norm(r, g2[...]).astype(BF16)

    def active(o, t):
        row[:, pl.ds(o, t.shape[1])] = 0.5 * t * (1.0 + lax.erf(t * (1.0 / math.sqrt(2.0))))

    by_columns(n, wfc1, 0, ff, active, compact)
    t = row[:, 0:ff].astype(BF16)
    by_columns(t, wfc2, 0, width, keep, compact)
    return (r + row[:, 0:width])[0:1, :].astype(BF16).astype(F32)


def first_kernel(
    patch_hbm, wqkv_hbm, wout_hbm, wfc1_hbm, wfc2_hbm, g1, g2,
    out_ref, turned, wqkv, wout, wfc1, wfc2, marks, blank, count,
    flat, norm, qkv, ctx, res, act, sems, *, images, toks,
):
    copies = [
        pltpu.make_async_copy(a, b, sems.at[k])
        for k, (a, b) in enumerate(((wqkv_hbm, wqkv), (wout_hbm, wout), (wfc1_hbm, wfc1), (wfc2_hbm, wfc2)))
    ]
    total = toks * images
    fetch = pltpu.make_async_copy(patch_hbm, flat.at[0:total, :], sems.at[4])
    section = lax.axis_index("section")
    pl.when(section == 0)(fetch.start)
    for c in copies:
        c.start()
    marks[...] = jnp.zeros_like(marks)
    blank[...] = jnp.zeros_like(blank)
    count[0] = 1

    @pl.when(section == 0)
    def _():
        span = flat.shape[0]
        flat[total:span, :] = jnp.zeros((span - total, flat.shape[1]), BF16)
        fetch.wait()
        take = WIDE // images
        r = lax.broadcasted_iota(jnp.int32, (WIDE, WIDE), 0)
        c = lax.broadcasted_iota(jnp.int32, (WIDE, WIDE), 1)
        order = (c == (r % take) * images + r // take).astype(F32).astype(BF16)
        rows = turned.shape[1]
        for k in range(0, rows, take):
            got = mm(order, flat[k * images : k * images + WIDE, :]).astype(BF16)
            size = min(take, rows - k)
            for i in range(images):
                turned[i, k : k + size, :] = got[i * take : i * take + size, :]
        x = turned[0].astype(F32)
        res[...] = x
        norm[...] = layer_norm(x, g1[...]).astype(BF16)
        encode(wqkv, wout, g2, wfc1, wfc2, out_ref, norm, qkv, ctx, res, act, toks, ready=lambda k: copies[k].wait())

    @pl.when(section != 0)
    def _():
        for c in copies:
            c.wait()


def first_tick(patches, weights, rows):
    images, toks, width = patches.shape
    g1, wqkv, wout, g2, wfc1, wfc2 = weights
    ff = wfc1.shape[1]
    whole = pl.BlockSpec(memory_space=pltpu.VMEM)
    hbm = pl.BlockSpec(memory_space=pl.ANY)
    span = -(-rows * images // WIDE) * WIDE
    return pl.pallas_call(
        functools.partial(first_kernel, images=images, toks=toks),
        out_shape=(
            pltpu.VMEM((rows, width), BF16),
            pltpu.VMEM((images, rows, width), BF16),
            pltpu.VMEM(wqkv.shape, BF16),
            pltpu.VMEM(wout.shape, BF16),
            pltpu.VMEM(wfc1.shape, BF16),
            pltpu.VMEM(wfc2.shape, BF16),
            pltpu.VMEM((images, width), F32),
            pltpu.VMEM((rows, width), BF16),
            pltpu.SMEM((1,), jnp.int32),
        ),
        in_specs=[hbm] * 5 + [whole] * 2,
        out_specs=(whole,) * 8 + (pl.BlockSpec(memory_space=pltpu.SMEM),),
        scratch_shapes=[
            pltpu.VMEM((span, width), BF16),
            pltpu.VMEM((rows, width), BF16),
            pltpu.VMEM((rows, 3 * width), BF16),
            pltpu.VMEM((rows, width), BF16),
            pltpu.VMEM((rows, width), F32),
            pltpu.VMEM((rows, ff), BF16),
            pltpu.SemaphoreType.DMA((5,)),
        ],
        compiler_params=pltpu.CompilerParams(vmem_limit_bytes=14 * 2**20),
        name="first",
    )(far(patches.transpose(1, 0, 2).reshape(toks * images, width)), far(wqkv), far(wout), far(wfc1), far(wfc2), g1, g2)


def tick_kernel(
    tick, turned, came, marks_in, g1, wqkv, wout, g2, wfc1, wfc2, out_ref, marks, after, norm, qkv, ctx, res, act, row, *, toks
):
    after[0] = tick[0] + 1
    section = lax.axis_index("section")
    last = lax.axis_size("section") - 1
    images = turned.shape[0]
    step = tick[0] - HOP * section
    active = jnp.logical_and(step >= 0, step < images)

    def start(x):
        res[...] = x
        norm[...] = layer_norm(x, g1[...]).astype(BF16)

    @pl.when(jnp.logical_and(active, section != last))
    def _():
        @pl.when(section == 0)
        def _():
            start(turned[step].astype(F32))

        @pl.when(section != 0)
        def _():
            start(came[...].astype(F32))

        encode(wqkv, wout, g2, wfc1, wfc2, out_ref, norm, qkv, ctx, res, act, toks)

    @pl.when(jnp.logical_and(active, section == last))
    def _():
        marks[pl.ds(step, 1), :] = encode_class(came, g1, wqkv, wout, g2, wfc1, wfc2, norm, qkv, row, toks, True)


def hold(x):
    return pltpu.with_memory_space_constraint(x, pltpu.VMEM)


def far(x):
    return pltpu.with_memory_space_constraint(x, pltpu.HBM)


def held_weights(weights):
    g1, wqkv, wout, g2, wfc1, wfc2 = weights
    return g1, hold(wqkv), hold(wout), g2, hold(wfc1), hold(wfc2)


def run_tick(tick, turned, came, marks, weights, toks):
    rows, width = came.shape
    ff = weights[4].shape[1]
    whole = pl.BlockSpec(memory_space=pltpu.VMEM)
    return pl.pallas_call(
        functools.partial(tick_kernel, toks=toks),
        out_shape=(pltpu.VMEM((rows, width), BF16), pltpu.VMEM(marks.shape, F32), pltpu.SMEM((1,), jnp.int32)),
        in_specs=[pl.BlockSpec(memory_space=pltpu.SMEM)] + [whole] * 9,
        out_specs=(whole, whole, pl.BlockSpec(memory_space=pltpu.SMEM)),
        scratch_shapes=[
            pltpu.VMEM((rows, width), BF16),
            pltpu.VMEM((rows, 3 * width), BF16),
            pltpu.VMEM((rows, width), BF16),
            pltpu.VMEM((rows, width), F32),
            pltpu.VMEM((rows, ff), BF16),
            pltpu.VMEM((8, max(ff, width)), F32),
        ],
        input_output_aliases={3: 1},
        compiler_params=pltpu.CompilerParams(vmem_limit_bytes=12 * 2**20),
        name="block",
    )(tick, hold(turned), hold(came), hold(marks), *held_weights(weights))


def merge_kernel(*refs):
    out_ref = refs[-1]
    size = refs[0].shape[0]
    for k, piece in enumerate(refs[:-1]):
        out_ref[k * size : (k + 1) * size, :] = piece[...]


def merge(*pieces):
    size, width = pieces[0].shape
    whole = pl.BlockSpec(memory_space=pltpu.VMEM)
    return pl.pallas_call(
        merge_kernel,
        out_shape=pltpu.VMEM((len(pieces) * size, width), pieces[0].dtype),
        in_specs=[whole] * len(pieces),
        out_specs=whole,
        compiler_params=pltpu.CompilerParams(vmem_limit_bytes=2**20),
        name="merge",
    )(*pieces)


def class_kernel(came, marks_in, g1, wqkv, wout, g2, wfc1, wfc2, marks, norm, qkv, row, *, toks):
    step = marks.shape[0] - 2

    @pl.when(lax.axis_index("section") == lax.axis_size("section") - 1)
    def _():
        marks[step : step + 1, :] = encode_class(came, g1, wqkv, wout, g2, wfc1, wfc2, norm, qkv, row, toks, True)


def run_class(came, marks, weights, toks):
    rows, width = came.shape
    whole = pl.BlockSpec(memory_space=pltpu.VMEM)
    return pl.pallas_call(
        functools.partial(class_kernel, toks=toks),
        out_shape=pltpu.VMEM(marks.shape, F32),
        in_specs=[whole] * 8,
        out_specs=whole,
        scratch_shapes=[
            pltpu.VMEM((rows, width), BF16),
            pltpu.VMEM((rows, width), BF16),
            pltpu.VMEM((8, max(weights[4].shape[1], width)), F32),
        ],
        input_output_aliases={1: 0},
        compiler_params=pltpu.CompilerParams(vmem_limit_bytes=12 * 2**20),
        name="class",
    )(hold(came), hold(marks), *held_weights(weights))


def straighten(swapped, ordered, images):
    group = lax.axis_index("dp")
    ordered[...] = jnp.zeros_like(ordered)
    for b in range(swapped.shape[0] // images):
        place = pl.multiple_of(jnp.bitwise_xor(group, b) * images, images)
        ordered[pl.ds(place, images), :] = swapped[b * images : (b + 1) * images, :].astype(F32)


def score_shard(fetch, back, out_ref, ordered, queue):
    lanes = out_ref.shape[1]
    fetch.wait()
    back.start()
    for k in range(out_ref.shape[0]):
        s = mm_t(queue[...], ordered[k * lanes : (k + 1) * lanes, :].astype(BF16)) * (1.0 / SHARPNESS)
        peak = jnp.max(s, axis=0, keepdims=True)
        out_ref[k : k + 1, :] = peak + jnp.log(jnp.sum(jnp.exp(s - peak), axis=0, keepdims=True))
    back.wait()


def early_kernel(swapped, queue_hbm, out_ref, copy_ref, query_ref, ordered, queue, sems, *, images):
    straighten(swapped, ordered, images)
    query_ref[...] = ordered[0 : query_ref.shape[0], :].astype(BF16)

    @pl.when(lax.axis_index("section") == lax.axis_size("section") - 1)
    def _():
        fetch = pltpu.make_async_copy(queue_hbm, queue, sems.at[0])
        back = pltpu.make_async_copy(queue, copy_ref, sems.at[1])
        fetch.start()
        score_shard(fetch, back, out_ref, ordered, queue)


def window_base(pointer, share, span):
    local = pointer[0] - lax.axis_index("section") * share
    return local, pl.multiple_of(jnp.clip((local // 16) * 16, 0, share - span), 16)


def late_kernel(
    query, queue_hbm, pointer, owner, lse_in, copy_in,
    out_ref, copy_ref, window, owner_ref, pointer_ref, ordered, queue, sems,
):
    share, span = queue_hbm.shape[0], window.shape[0]
    pointer_ref[0] = pointer[0]
    owner_ref[...] = owner[...]
    _, base = window_base(pointer, share, span)
    bring = pltpu.make_async_copy(queue_hbm.at[pl.ds(base, span), :], window, sems.at[2])
    bring.start()

    @pl.when(lax.axis_index("section") != lax.axis_size("section") - 1)
    def _():
        fetch = pltpu.make_async_copy(queue_hbm, queue, sems.at[0])
        back = pltpu.make_async_copy(queue, copy_ref, sems.at[1])
        fetch.start()
        ordered[...] = jnp.zeros_like(ordered)
        ordered[0 : query.shape[0], :] = query[...].astype(F32)
        score_shard(fetch, back, out_ref, ordered, queue)

    @pl.when(lax.axis_index("section") == lax.axis_size("section") - 1)
    def _():
        out_ref[...] = lse_in[...]

    bring.wait()


def head_kernel(came, marks, g1, wqkv, wout, g2, wfc1, wfc2, gain, head, lse, out_ref, found, norm, qkv, row, *, toks):
    images = found.shape[0]

    @pl.when(lax.axis_index("section") == lax.axis_size("section") - 1)
    def _():
        found[...] = marks[...]
        found[images - 1 : images, :] = encode_class(came, g1, wqkv, wout, g2, wfc1, wfc2, norm, qkv, row, toks, False)

    @pl.when(lax.axis_index("section") != lax.axis_size("section") - 1)
    def _():
        found[...] = jnp.zeros_like(found)

    normed = layer_norm(found[...], gain[...]).astype(BF16)
    z = mm(normed, head[...])
    z = z * lax.rsqrt(1.0 + jnp.sum(z * z, axis=1, keepdims=True))
    kd = z.shape[1]
    peers, rows, lanes = out_ref.shape
    parts = [z[:, o : o + lanes] for o in range(0, kd, lanes)]
    high = lse[...].astype(BF16).astype(F32)
    mid = (lse[...] - high).astype(BF16).astype(F32)
    low = lse[...] - high - mid
    parts += [high, mid, low]
    used = sum(p.shape[0] for p in parts)
    if rows > used:
        parts.append(jnp.zeros((rows - used, lanes), F32))
    block = jnp.concatenate(parts, axis=0).astype(BF16)
    out_ref[...] = jnp.broadcast_to(block[None], out_ref.shape)


def final_kernel(
    pointer, got, query, owner, window, queue_in, keys_ref, loss_ref, total_ref, queue_ref, merged, sem, *, images, kd
):
    section = lax.axis_index("section")
    group = lax.axis_index("dp")
    span = window.shape[0]
    local, base = window_base(pointer, queue_ref.shape[0], span)
    extra = -(-query.shape[0] // got.shape[2])
    peers, rows, lanes = got.shape
    halves = kd // lanes
    count = query.shape[0]
    n_sec = peers * images // count
    pieces = []
    for g in range(count // images):
        src = g * n_sec + n_sec - 1
        one = got[src].astype(F32)
        pieces.append(jnp.concatenate([one[h * images : (h + 1) * images] for h in range(halves)], axis=1))
    keys = jnp.concatenate(pieces, axis=0)
    keys16 = keys.astype(BF16)
    row = lax.broadcasted_iota(jnp.int32, (span, count), 0) + (base - local)
    slot = owner[...] - group * images
    pick = jnp.logical_and(row == slot, jnp.logical_and(slot >= 0, slot < images))
    fresh = mm(pick.astype(F32).astype(BF16), keys16)
    hit = jnp.sum(pick.astype(F32), axis=1, keepdims=True) > 0.5
    merged[...] = jnp.where(hit, fresh, window[...].astype(F32)).astype(BF16)
    back = pltpu.make_async_copy(merged, queue_ref.at[pl.ds(base, span), :], sem)
    back.start()
    msgs = got[...].astype(F32)
    off = halves * images
    lse = msgs[:, off : off + extra, :] + msgs[:, off + extra : off + 2 * extra, :] + msgs[:, off + 2 * extra : off + 3 * extra, :]
    peak = jnp.max(lse, axis=0)
    negative = peak + jnp.log(jnp.sum(jnp.exp(lse - peak[None]), axis=0))
    square = mm_t(query[...], keys16)
    r = lax.broadcasted_iota(jnp.int32, square.shape, 0)
    c = lax.broadcasted_iota(jnp.int32, square.shape, 1)
    positive = jnp.sum(jnp.where(r == c, square, 0.0), axis=0, keepdims=True) * (1.0 / SHARPNESS)
    positive = jnp.pad(positive, ((0, 0), (0, lanes - count)))
    larger = jnp.maximum(negative, positive)
    loss = larger + jnp.log(jnp.exp(negative - larger) + jnp.exp(positive - larger)) - positive
    lane = lax.broadcasted_iota(jnp.int32, loss.shape, 1)
    total_ref[...] = jnp.sum(jnp.where(lane < count, loss, 0.0), axis=1, keepdims=True) * (1.0 / count)
    turned = pltpu.roll(jnp.broadcast_to(loss, (8, lanes)), lanes - group * images, 1)
    loss_ref[...] = turned[0:1, 0:images]
    mine = got[group * n_sec + n_sec - 1].astype(F32)
    keys_ref[...] = jnp.concatenate([mine[h * images : (h + 1) * images] for h in range(halves)], axis=1).astype(BF16)
    back.wait()


def on_device(
    patches,
    ln1_gain,
    w_qkv,
    w_out,
    ln2_gain,
    w_fc1,
    w_fc2,
    final_norm_gain,
    w_head,
    online_embeddings,
    queue,
    owner,
    pointer,
):
    sections = lax.axis_size("section")
    groups = lax.axis_size("dp")
    section = lax.axis_index("section").astype(jnp.int32)
    group = lax.axis_index("dp").astype(jnp.int32)
    images, toks, width = patches.shape
    kd = w_head.shape[1]
    peers = sections * groups
    count = groups * images
    rows = -(-toks // 8) * 8
    whole = pl.BlockSpec(memory_space=pltpu.VMEM)
    smem = pl.BlockSpec(memory_space=pltpu.SMEM)
    hbm = pl.BlockSpec(memory_space=pl.ANY)

    extra = -(-count // LANES)
    limit = pltpu.CompilerParams(vmem_limit_bytes=4 * 2**20)
    shapes = (pltpu.VMEM((extra, LANES), F32), jax.ShapeDtypeStruct(queue.shape, BF16))
    work = [
        pltpu.VMEM((extra * LANES, kd), F32),
        pltpu.VMEM(queue.shape, BF16),
        pltpu.SemaphoreType.DMA((3,)),
    ]
    chain = [(k, k + 1) for k in range(sections - 1)]
    ticks = images + HOP * (sections - 1)
    def exchange(rows, hop):
        pairs = [(k * sections + j, (k ^ hop) * sections + j) for k in range(groups) for j in range(sections)]
        return lax.ppermute(rows, ("dp", "section"), pairs)

    swapped = online_embeddings
    other = exchange(swapped, 1)
    sent, turned, *held, marks, blank, tick = first_tick(
        patches, (ln1_gain, w_qkv[0], w_out[0], ln2_gain, w_fc1[0], w_fc2[0]), rows
    )
    weights = (ln1_gain, held[0], held[1], ln2_gain, held[2], held[3])
    loops = ticks - 4
    unroll = next(k for k in (2, 1) if loops % k == 0)

    def one(tick, came, sent, marks):
        coming = lax.ppermute(sent, "section", chain)
        sent, marks, tick = run_tick(tick, turned, came, marks, weights, toks)
        return tick, coming, sent, marks

    def advance(carry):
        for _ in range(unroll):
            carry = one(*carry)
        return carry

    other, sent = lax.optimization_barrier((other, sent))
    swapped = merge(swapped, other)
    near = [hop for hop in (2, 4, 6) if hop < groups]
    others = [exchange(swapped, hop) for hop in near]
    tick, came, sent, marks = one(tick, blank, sent, marks)
    *others, sent = lax.optimization_barrier((*others, sent))
    swapped = merge(swapped, *others)
    hop = 8
    while hop < groups:
        swapped = merge(swapped, exchange(swapped, hop))
        hop *= 2
    lse, queue_copy, query = pl.pallas_call(
        functools.partial(early_kernel, images=images),
        out_shape=shapes + (pltpu.VMEM((count, kd), BF16),),
        in_specs=[whole, hbm],
        out_specs=(whole, hbm, whole),
        scratch_shapes=work,
        compiler_params=limit,
        name="early",
    )(hold(swapped), far(queue))
    lse, sent = lax.optimization_barrier((lse, sent))
    carry = lax.while_loop(lambda carry: carry[0][0] <= loops + 1, advance, (tick, came, sent, marks))
    _, came, sent, marks = carry
    coming = lax.ppermute(sent, "section", chain[-1:])
    marks = run_class(came, marks, weights, toks)
    came = coming

    lse, marks = lax.optimization_barrier((lse, marks))
    lse, queue_copy, window, owner_row, start = pl.pallas_call(
        late_kernel,
        out_shape=shapes
        + (
            pltpu.VMEM((32, kd), BF16),
            pltpu.VMEM((1, count), jnp.int32),
            pltpu.SMEM((1,), jnp.int32),
        ),
        in_specs=[whole, hbm, smem, whole, whole, hbm],
        out_specs=(whole, hbm, whole, whole, smem),
        scratch_shapes=work,
        input_output_aliases={5: 1},
        compiler_params=limit,
        name="late",
    )(hold(query), far(queue), pointer, owner.reshape(1, count), hold(lse), far(queue_copy))
    height = -(-(kd // LANES * images + 3 * extra) // 8) * 8
    message = pl.pallas_call(
        functools.partial(head_kernel, toks=toks),
        out_shape=jax.ShapeDtypeStruct((peers, height, LANES), BF16),
        in_specs=[whole] * 11,
        out_specs=whole,
        scratch_shapes=[
            pltpu.VMEM((images, width), F32),
            pltpu.VMEM((rows, width), BF16),
            pltpu.VMEM((rows, 3 * width), BF16),
            pltpu.VMEM((8, max(w_fc1.shape[2], width)), F32),
        ],
        compiler_params=pltpu.CompilerParams(vmem_limit_bytes=12 * 2**20),
        name="head",
    )(hold(came), hold(marks), *held_weights(weights), final_norm_gain.reshape(1, width), w_head, hold(lse))
    got = lax.all_to_all(message, ("dp", "section"), 0, 0, tiled=True)

    keys, loss, total, new_queue = pl.pallas_call(
        functools.partial(final_kernel, images=images, kd=kd),
        out_shape=(
            jax.ShapeDtypeStruct((images, kd), BF16),
            jax.ShapeDtypeStruct((1, images), F32),
            jax.ShapeDtypeStruct((1, 1), F32),
            jax.ShapeDtypeStruct(queue.shape, BF16),
        ),
        in_specs=[smem, whole, whole, whole, whole, hbm],
        out_specs=(whole, whole, whole, hbm),
        scratch_shapes=[pltpu.VMEM((32, kd), BF16), pltpu.SemaphoreType.DMA],
        input_output_aliases={5: 3},
        name="final",
    )(start, hold(got), hold(query), hold(owner_row), hold(window), far(queue_copy))
    return keys, loss.reshape(images), total.reshape(()), new_queue


def solution(mesh):
    placed = (
        P("dp", None, None),
        P("section", None),
        P("section", None, None),
        P("section", None, None),
        P("section", None),
        P("section", None, None),
        P("section", None, None),
        P(),
        P(),
        P("dp", None),
        P(("dp", "section"), None),
        P(),
        P("dp"),
    )
    return jax.shard_map(
        on_device,
        mesh=mesh,
        in_specs=placed,
        out_specs=(P("dp", None), P("dp"), P(), P(("dp", "section"), None)),
        check_vma=False,
    )
```

```python
import functools
import math

import jax
import jax.numpy as jnp
from jax import lax
from jax.experimental import pallas as pl
from jax.experimental.pallas import tpu as pltpu
from jax.sharding import PartitionSpec as P

F32 = jnp.float32
BF16 = jnp.bfloat16
HEAD_DIM = 64
LANES = 128
WIDE = 256
SHARPNESS = 0.2
HOP = 2


def layer_norm(values, gain):
    center = values - jnp.mean(values, axis=-1, keepdims=True)
    spread = jnp.mean(center * center, axis=-1, keepdims=True)
    return center * lax.rsqrt(spread + 1e-06) * gain


def mm(left, right):
    return jnp.dot(left, right, preferred_element_type=F32)


def mm_t(left, right):
    return lax.dot_general(left, right, (((1,), (1,)), ((), ())), preferred_element_type=F32)


def attention_tools(rows, toks):
    pair = LANES // HEAD_DIM
    lane = lax.broadcasted_iota(jnp.int32, (rows, LANES), 1) // HEAD_DIM
    keep = lax.broadcasted_iota(jnp.int32, (rows, rows), 1) < toks
    return pair, lane, keep


def encode(wqkv, wout, g2, wfc1, wfc2, out_ref, norm, qkv, ctx, res, act, toks, ready=None):
    rows, width = norm.shape
    ff = wfc1.shape[1]
    quad = WIDE // HEAD_DIM
    pair, lane, keep = attention_tools(rows, toks)
    scale = 1.0 / math.sqrt(HEAD_DIM)
    ready = ready or (lambda k: None)

    def project(j):
        for part in range(3):
            o = part * width + j * WIDE
            y = mm(norm[...], wqkv[:, o : o + WIDE])
            if part == 0:
                y = y * scale
            qkv[:, o : o + WIDE] = y.astype(BF16)

    def scores(j):
        found = []
        for h in range(quad):
            o = j * WIDE + (h // pair) * LANES
            q = qkv[:, o : o + LANES]
            q = jnp.where(lane == h % pair, q, jnp.zeros_like(q))
            found.append(mm_t(q, qkv[:, width + o : width + o + LANES]))
        return found

    def soften(found):
        out = []
        for s in found:
            s = jnp.where(keep, s, -1e30)
            out.append(jnp.exp(s - jnp.max(s, axis=-1, keepdims=True)).astype(BF16))
        return out

    def mix(j, weights):
        ones = jnp.ones((rows, LANES), BF16)
        for half in range(quad // pair):
            o = j * WIDE + half * LANES
            v = jnp.concatenate([qkv[:, 2 * width + o : 2 * width + o + LANES], ones], axis=1)
            got = None
            for i in range(pair):
                y = mm(weights[half * pair + i], v)
                y = y[:, :LANES] / y[:, LANES:]
                got = y if got is None else jnp.where(lane == i, y, got)
            ctx[:, o : o + LANES] = got.astype(BF16)

    groups = width // WIDE
    late = (groups - 1) * WIDE
    ready(0)
    project(0)
    if groups > 1:
        project(1)
    found = scores(0)
    for j in range(groups):
        coming = None
        if j + 1 < groups:
            coming = scores(j + 1)
        if j + 2 < groups:
            project(j + 2)
        if j + 1 == groups:
            ready(1)
            for n in range(0, width, WIDE):
                res[:, n : n + WIDE] += mm(ctx[:, 0:late], wout[0:late, n : n + WIDE])
        mix(j, soften(found))
        found = coming
    for n in range(0, width, WIDE):
        res[:, n : n + WIDE] += mm(ctx[:, late:width], wout[late:width, n : n + WIDE])
    norm[...] = layer_norm(res[...], g2[...]).astype(BF16)
    ready(2)
    for n in range(0, ff, WIDE):
        t = mm(norm[...], wfc1[:, n : n + WIDE])
        t = 0.5 * t * (1.0 + lax.erf(t * (1.0 / math.sqrt(2.0))))
        act[:, n : n + WIDE] = t.astype(BF16)
    ready(3)
    for n in range(0, width, WIDE):
        out_ref[:, n : n + WIDE] = (res[:, n : n + WIDE] + mm(act[...], wfc2[:, n : n + WIDE])).astype(BF16)


def by_columns(left, right, start, stop, store, compact):
    size = 2 * WIDE if compact else WIDE

    def part(o):
        store(o - start, mm(left, right[:, pl.ds(o, size)]))

    if compact:
        lax.fori_loop(start // size, stop // size, lambda k, _: (part(pl.multiple_of(k * size, size)), 0)[1], 0)
    else:
        for o in range(start, stop, size):
            part(o)


def encode_class(x_ref, g1, wqkv, wout, g2, wfc1, wfc2, norm, qkv, row, toks, compact):
    rows, width = norm.shape
    ff = wfc1.shape[1]
    heads = width // HEAD_DIM
    scale = 1.0 / math.sqrt(HEAD_DIM)
    norm[...] = layer_norm(x_ref[...].astype(F32), g1[...]).astype(BF16)

    def keep(o, y):
        row[:, pl.ds(o, y.shape[1])] = y

    by_columns(norm[0:8, :], wqkv, 0, width, keep, compact)
    q = row[0:1, 0:width] * scale
    own = lax.broadcasted_iota(jnp.int32, (heads, width), 1) // HEAD_DIM
    own = own == lax.broadcasted_iota(jnp.int32, (heads, width), 0)
    q = jnp.where(own, jnp.broadcast_to(q, (heads, width)), 0.0).astype(BF16)

    def keys(o, y):
        qkv[:, pl.ds(o, y.shape[1])] = y.astype(BF16)

    by_columns(norm[...], wqkv, width, 2 * width, keys, compact)
    s = mm_t(q, qkv[:, 0:width])
    s = jnp.where(lax.broadcasted_iota(jnp.int32, s.shape, 1) < toks, s, -1e30)
    e = jnp.exp(s - jnp.max(s, axis=-1, keepdims=True))
    p = (e / jnp.sum(e, axis=-1, keepdims=True)).astype(BF16)
    mixed = mm(p, norm[...]).astype(BF16)

    def values(o, y):
        lane = lax.broadcasted_iota(jnp.int32, y.shape, 1) + o
        mine = lane // HEAD_DIM == lax.broadcasted_iota(jnp.int32, y.shape, 0)
        y = jnp.sum(jnp.where(mine, y, 0.0), axis=0, keepdims=True)
        row[:, pl.ds(o, y.shape[1])] = jnp.broadcast_to(y, (8, y.shape[1]))

    by_columns(mixed, wqkv, 2 * width, 3 * width, values, compact)
    c = row[:, 0:width].astype(BF16)
    by_columns(c, wout, 0, width, keep, compact)
    r = x_ref[0:8, :].astype(F32) + row[:, 0:width]
    n = layer_norm(r, g2[...]).astype(BF16)

    def active(o, t):
        row[:, pl.ds(o, t.shape[1])] = 0.5 * t * (1.0 + lax.erf(t * (1.0 / math.sqrt(2.0))))

    by_columns(n, wfc1, 0, ff, active, compact)
    t = row[:, 0:ff].astype(BF16)
    by_columns(t, wfc2, 0, width, keep, compact)
    return (r + row[:, 0:width])[0:1, :].astype(BF16).astype(F32)


def first_kernel(
    patch_hbm, wqkv_hbm, wout_hbm, wfc1_hbm, wfc2_hbm, g1, g2,
    out_ref, turned, wqkv, wout, wfc1, wfc2, marks, blank, count,
    flat, norm, qkv, ctx, res, act, sems, *, images, toks,
):
    copies = [
        pltpu.make_async_copy(a, b, sems.at[k])
        for k, (a, b) in enumerate(((wqkv_hbm, wqkv), (wout_hbm, wout), (wfc1_hbm, wfc1), (wfc2_hbm, wfc2)))
    ]
    total = toks * images
    fetch = pltpu.make_async_copy(patch_hbm, flat.at[0:total, :], sems.at[4])
    section = lax.axis_index("section")
    pl.when(section == 0)(fetch.start)
    for c in copies:
        c.start()
    marks[...] = jnp.zeros_like(marks)
    blank[...] = jnp.zeros_like(blank)
    count[0] = 1

    @pl.when(section == 0)
    def _():
        span = flat.shape[0]
        flat[total:span, :] = jnp.zeros((span - total, flat.shape[1]), BF16)
        fetch.wait()
        take = WIDE // images
        r = lax.broadcasted_iota(jnp.int32, (WIDE, WIDE), 0)
        c = lax.broadcasted_iota(jnp.int32, (WIDE, WIDE), 1)
        order = (c == (r % take) * images + r // take).astype(F32).astype(BF16)
        rows = turned.shape[1]
        for k in range(0, rows, take):
            got = mm(order, flat[k * images : k * images + WIDE, :]).astype(BF16)
            size = min(take, rows - k)
            for i in range(images):
                turned[i, k : k + size, :] = got[i * take : i * take + size, :]
        x = turned[0].astype(F32)
        res[...] = x
        norm[...] = layer_norm(x, g1[...]).astype(BF16)
        encode(wqkv, wout, g2, wfc1, wfc2, out_ref, norm, qkv, ctx, res, act, toks, ready=lambda k: copies[k].wait())

    @pl.when(section != 0)
    def _():
        for c in copies:
            c.wait()


def first_tick(patches, weights, rows):
    images, toks, width = patches.shape
    g1, wqkv, wout, g2, wfc1, wfc2 = weights
    ff = wfc1.shape[1]
    whole = pl.BlockSpec(memory_space=pltpu.VMEM)
    hbm = pl.BlockSpec(memory_space=pl.ANY)
    span = -(-rows * images // WIDE) * WIDE
    return pl.pallas_call(
        functools.partial(first_kernel, images=images, toks=toks),
        out_shape=(
            pltpu.VMEM((rows, width), BF16),
            pltpu.VMEM((images, rows, width), BF16),
            pltpu.VMEM(wqkv.shape, BF16),
            pltpu.VMEM(wout.shape, BF16),
            pltpu.VMEM(wfc1.shape, BF16),
            pltpu.VMEM(wfc2.shape, BF16),
            pltpu.VMEM((images, width), F32),
            pltpu.VMEM((rows, width), BF16),
            pltpu.SMEM((1,), jnp.int32),
        ),
        in_specs=[hbm] * 5 + [whole] * 2,
        out_specs=(whole,) * 8 + (pl.BlockSpec(memory_space=pltpu.SMEM),),
        scratch_shapes=[
            pltpu.VMEM((span, width), BF16),
            pltpu.VMEM((rows, width), BF16),
            pltpu.VMEM((rows, 3 * width), BF16),
            pltpu.VMEM((rows, width), BF16),
            pltpu.VMEM((rows, width), F32),
            pltpu.VMEM((rows, ff), BF16),
            pltpu.SemaphoreType.DMA((5,)),
        ],
        compiler_params=pltpu.CompilerParams(vmem_limit_bytes=14 * 2**20),
        name="first",
    )(far(patches.transpose(1, 0, 2).reshape(toks * images, width)), far(wqkv), far(wout), far(wfc1), far(wfc2), g1, g2)


def tick_kernel(
    tick, turned, came, marks_in, g1, wqkv, wout, g2, wfc1, wfc2, out_ref, marks, after, norm, qkv, ctx, res, act, row, *, toks
):
    after[0] = tick[0] + 1
    section = lax.axis_index("section")
    last = lax.axis_size("section") - 1
    images = turned.shape[0]
    step = tick[0] - HOP * section
    active = jnp.logical_and(step >= 0, step < images)

    def start(x):
        res[...] = x
        norm[...] = layer_norm(x, g1[...]).astype(BF16)

    @pl.when(jnp.logical_and(active, section != last))
    def _():
        @pl.when(section == 0)
        def _():
            start(turned[step].astype(F32))

        @pl.when(section != 0)
        def _():
            start(came[...].astype(F32))

        encode(wqkv, wout, g2, wfc1, wfc2, out_ref, norm, qkv, ctx, res, act, toks)

    @pl.when(jnp.logical_and(active, section == last))
    def _():
        marks[pl.ds(step, 1), :] = encode_class(came, g1, wqkv, wout, g2, wfc1, wfc2, norm, qkv, row, toks, True)


def hold(x):
    return pltpu.with_memory_space_constraint(x, pltpu.VMEM)


def far(x):
    return pltpu.with_memory_space_constraint(x, pltpu.HBM)


def held_weights(weights):
    g1, wqkv, wout, g2, wfc1, wfc2 = weights
    return g1, hold(wqkv), hold(wout), g2, hold(wfc1), hold(wfc2)


def run_tick(tick, turned, came, marks, weights, toks):
    rows, width = came.shape
    ff = weights[4].shape[1]
    whole = pl.BlockSpec(memory_space=pltpu.VMEM)
    return pl.pallas_call(
        functools.partial(tick_kernel, toks=toks),
        out_shape=(pltpu.VMEM((rows, width), BF16), pltpu.VMEM(marks.shape, F32), pltpu.SMEM((1,), jnp.int32)),
        in_specs=[pl.BlockSpec(memory_space=pltpu.SMEM)] + [whole] * 9,
        out_specs=(whole, whole, pl.BlockSpec(memory_space=pltpu.SMEM)),
        scratch_shapes=[
            pltpu.VMEM((rows, width), BF16),
            pltpu.VMEM((rows, 3 * width), BF16),
            pltpu.VMEM((rows, width), BF16),
            pltpu.VMEM((rows, width), F32),
            pltpu.VMEM((rows, ff), BF16),
            pltpu.VMEM((8, max(ff, width)), F32),
        ],
        input_output_aliases={3: 1},
        compiler_params=pltpu.CompilerParams(vmem_limit_bytes=12 * 2**20),
        name="block",
    )(tick, hold(turned), hold(came), hold(marks), *held_weights(weights))


def merge_kernel(*refs):
    out_ref = refs[-1]
    size = refs[0].shape[0]
    for k, piece in enumerate(refs[:-1]):
        out_ref[k * size : (k + 1) * size, :] = piece[...]


def merge(*pieces):
    size, width = pieces[0].shape
    whole = pl.BlockSpec(memory_space=pltpu.VMEM)
    return pl.pallas_call(
        merge_kernel,
        out_shape=pltpu.VMEM((len(pieces) * size, width), pieces[0].dtype),
        in_specs=[whole] * len(pieces),
        out_specs=whole,
        compiler_params=pltpu.CompilerParams(vmem_limit_bytes=2**20),
        name="merge",
    )(*pieces)


def class_kernel(came, marks_in, g1, wqkv, wout, g2, wfc1, wfc2, marks, norm, qkv, row, *, toks):
    step = marks.shape[0] - 2

    @pl.when(lax.axis_index("section") == lax.axis_size("section") - 1)
    def _():
        marks[step : step + 1, :] = encode_class(came, g1, wqkv, wout, g2, wfc1, wfc2, norm, qkv, row, toks, False)


def run_class(came, marks, weights, toks):
    rows, width = came.shape
    whole = pl.BlockSpec(memory_space=pltpu.VMEM)
    return pl.pallas_call(
        functools.partial(class_kernel, toks=toks),
        out_shape=pltpu.VMEM(marks.shape, F32),
        in_specs=[whole] * 8,
        out_specs=whole,
        scratch_shapes=[
            pltpu.VMEM((rows, width), BF16),
            pltpu.VMEM((rows, width), BF16),
            pltpu.VMEM((8, max(weights[4].shape[1], width)), F32),
        ],
        input_output_aliases={1: 0},
        compiler_params=pltpu.CompilerParams(vmem_limit_bytes=12 * 2**20),
        name="class",
    )(hold(came), hold(marks), *held_weights(weights))


def straighten(swapped, ordered, images):
    group = lax.axis_index("dp")
    ordered[...] = jnp.zeros_like(ordered)
    for b in range(swapped.shape[0] // images):
        place = pl.multiple_of(jnp.bitwise_xor(group, b) * images, images)
        ordered[pl.ds(place, images), :] = swapped[b * images : (b + 1) * images, :].astype(F32)


def score_shard(fetch, back, out_ref, ordered, queue):
    lanes = out_ref.shape[1]
    fetch.wait()
    back.start()
    for k in range(out_ref.shape[0]):
        s = mm_t(queue[...], ordered[k * lanes : (k + 1) * lanes, :].astype(BF16)) * (1.0 / SHARPNESS)
        peak = jnp.max(s, axis=0, keepdims=True)
        out_ref[k : k + 1, :] = peak + jnp.log(jnp.sum(jnp.exp(s - peak), axis=0, keepdims=True))
    back.wait()


def early_kernel(swapped, queue_hbm, out_ref, copy_ref, query_ref, ordered, queue, sems, *, images):
    straighten(swapped, ordered, images)
    query_ref[...] = ordered[0 : query_ref.shape[0], :].astype(BF16)

    @pl.when(lax.axis_index("section") == lax.axis_size("section") - 1)
    def _():
        fetch = pltpu.make_async_copy(queue_hbm, queue, sems.at[0])
        back = pltpu.make_async_copy(queue, copy_ref, sems.at[1])
        fetch.start()
        score_shard(fetch, back, out_ref, ordered, queue)


def window_base(pointer, share, span):
    local = pointer[0] - lax.axis_index("section") * share
    return local, pl.multiple_of(jnp.clip((local // 16) * 16, 0, share - span), 16)


def late_kernel(
    query, queue_hbm, pointer, owner, lse_in, copy_in,
    out_ref, copy_ref, window, owner_ref, pointer_ref, ordered, queue, sems,
):
    share, span = queue_hbm.shape[0], window.shape[0]
    pointer_ref[0] = pointer[0]
    owner_ref[...] = owner[...]
    _, base = window_base(pointer, share, span)
    bring = pltpu.make_async_copy(queue_hbm.at[pl.ds(base, span), :], window, sems.at[2])
    bring.start()

    @pl.when(lax.axis_index("section") != lax.axis_size("section") - 1)
    def _():
        fetch = pltpu.make_async_copy(queue_hbm, queue, sems.at[0])
        back = pltpu.make_async_copy(queue, copy_ref, sems.at[1])
        fetch.start()
        ordered[...] = jnp.zeros_like(ordered)
        ordered[0 : query.shape[0], :] = query[...].astype(F32)
        score_shard(fetch, back, out_ref, ordered, queue)

    @pl.when(lax.axis_index("section") == lax.axis_size("section") - 1)
    def _():
        out_ref[...] = lse_in[...]

    bring.wait()


def head_kernel(came, marks, g1, wqkv, wout, g2, wfc1, wfc2, gain, head, lse, out_ref, found, norm, qkv, row, *, toks):
    images = found.shape[0]

    @pl.when(lax.axis_index("section") == lax.axis_size("section") - 1)
    def _():
        found[...] = marks[...]
        found[images - 1 : images, :] = encode_class(came, g1, wqkv, wout, g2, wfc1, wfc2, norm, qkv, row, toks, False)

    @pl.when(lax.axis_index("section") != lax.axis_size("section") - 1)
    def _():
        found[...] = jnp.zeros_like(found)

    normed = layer_norm(found[...], gain[...]).astype(BF16)
    z = mm(normed, head[...])
    z = z * lax.rsqrt(1.0 + jnp.sum(z * z, axis=1, keepdims=True))
    kd = z.shape[1]
    peers, rows, lanes = out_ref.shape
    parts = [z[:, o : o + lanes] for o in range(0, kd, lanes)]
    high = lse[...].astype(BF16).astype(F32)
    mid = (lse[...] - high).astype(BF16).astype(F32)
    low = lse[...] - high - mid
    parts += [high, mid, low]
    used = sum(p.shape[0] for p in parts)
    if rows > used:
        parts.append(jnp.zeros((rows - used, lanes), F32))
    block = jnp.concatenate(parts, axis=0).astype(BF16)
    out_ref[...] = jnp.broadcast_to(block[None], out_ref.shape)


def final_kernel(
    pointer, got, query, owner, window, queue_in, keys_ref, loss_ref, total_ref, queue_ref, merged, sem, *, images, kd
):
    section = lax.axis_index("section")
    group = lax.axis_index("dp")
    span = window.shape[0]
    local, base = window_base(pointer, queue_ref.shape[0], span)
    extra = -(-query.shape[0] // got.shape[2])
    peers, rows, lanes = got.shape
    halves = kd // lanes
    count = query.shape[0]
    n_sec = peers * images // count
    pieces = []
    for g in range(count // images):
        src = g * n_sec + n_sec - 1
        one = got[src].astype(F32)
        pieces.append(jnp.concatenate([one[h * images : (h + 1) * images] for h in range(halves)], axis=1))
    keys = jnp.concatenate(pieces, axis=0)
    keys16 = keys.astype(BF16)
    row = lax.broadcasted_iota(jnp.int32, (span, count), 0) + (base - local)
    slot = owner[...] - group * images
    pick = jnp.logical_and(row == slot, jnp.logical_and(slot >= 0, slot < images))
    fresh = mm(pick.astype(F32).astype(BF16), keys16)
    hit = jnp.sum(pick.astype(F32), axis=1, keepdims=True) > 0.5
    merged[...] = jnp.where(hit, fresh, window[...].astype(F32)).astype(BF16)
    back = pltpu.make_async_copy(merged, queue_ref.at[pl.ds(base, span), :], sem)
    back.start()
    msgs = got[...].astype(F32)
    off = halves * images
    lse = msgs[:, off : off + extra, :] + msgs[:, off + extra : off + 2 * extra, :] + msgs[:, off + 2 * extra : off + 3 * extra, :]
    peak = jnp.max(lse, axis=0)
    negative = peak + jnp.log(jnp.sum(jnp.exp(lse - peak[None]), axis=0))
    square = mm_t(query[...], keys16)
    r = lax.broadcasted_iota(jnp.int32, square.shape, 0)
    c = lax.broadcasted_iota(jnp.int32, square.shape, 1)
    positive = jnp.sum(jnp.where(r == c, square, 0.0), axis=0, keepdims=True) * (1.0 / SHARPNESS)
    positive = jnp.pad(positive, ((0, 0), (0, lanes - count)))
    larger = jnp.maximum(negative, positive)
    loss = larger + jnp.log(jnp.exp(negative - larger) + jnp.exp(positive - larger)) - positive
    lane = lax.broadcasted_iota(jnp.int32, loss.shape, 1)
    total_ref[...] = jnp.sum(jnp.where(lane < count, loss, 0.0), axis=1, keepdims=True) * (1.0 / count)
    turned = pltpu.roll(jnp.broadcast_to(loss, (8, lanes)), lanes - group * images, 1)
    loss_ref[...] = turned[0:1, 0:images]
    mine = got[group * n_sec + n_sec - 1].astype(F32)
    keys_ref[...] = jnp.concatenate([mine[h * images : (h + 1) * images] for h in range(halves)], axis=1).astype(BF16)
    back.wait()


def on_device(
    patches,
    ln1_gain,
    w_qkv,
    w_out,
    ln2_gain,
    w_fc1,
    w_fc2,
    final_norm_gain,
    w_head,
    online_embeddings,
    queue,
    owner,
    pointer,
):
    sections = lax.axis_size("section")
    groups = lax.axis_size("dp")
    section = lax.axis_index("section").astype(jnp.int32)
    group = lax.axis_index("dp").astype(jnp.int32)
    images, toks, width = patches.shape
    kd = w_head.shape[1]
    peers = sections * groups
    count = groups * images
    rows = -(-toks // 8) * 8
    whole = pl.BlockSpec(memory_space=pltpu.VMEM)
    smem = pl.BlockSpec(memory_space=pltpu.SMEM)
    hbm = pl.BlockSpec(memory_space=pl.ANY)

    extra = -(-count // LANES)
    limit = pltpu.CompilerParams(vmem_limit_bytes=4 * 2**20)
    shapes = (pltpu.VMEM((extra, LANES), F32), jax.ShapeDtypeStruct(queue.shape, BF16))
    work = [
        pltpu.VMEM((extra * LANES, kd), F32),
        pltpu.VMEM(queue.shape, BF16),
        pltpu.SemaphoreType.DMA((3,)),
    ]
    chain = [(k, k + 1) for k in range(sections - 1)]
    ticks = images + HOP * (sections - 1)
    def exchange(rows, hop):
        pairs = [(k * sections + j, (k ^ hop) * sections + j) for k in range(groups) for j in range(sections)]
        return lax.ppermute(rows, ("dp", "section"), pairs)

    swapped = online_embeddings
    other = exchange(swapped, 1)
    sent, turned, *held, marks, blank, tick = first_tick(
        patches, (ln1_gain, w_qkv[0], w_out[0], ln2_gain, w_fc1[0], w_fc2[0]), rows
    )
    weights = (ln1_gain, held[0], held[1], ln2_gain, held[2], held[3])
    loops = ticks - 4
    unroll = next(k for k in (2, 1) if loops % k == 0)

    def one(tick, came, sent, marks):
        coming = lax.ppermute(sent, "section", chain)
        sent, marks, tick = run_tick(tick, turned, came, marks, weights, toks)
        return tick, coming, sent, marks

    def advance(carry):
        for _ in range(unroll):
            carry = one(*carry)
        return carry

    other, sent = lax.optimization_barrier((other, sent))
    swapped = merge(swapped, other)
    near = [hop for hop in (2, 4, 6) if hop < groups]
    others = [exchange(swapped, hop) for hop in near]
    tick, came, sent, marks = one(tick, blank, sent, marks)
    *others, sent = lax.optimization_barrier((*others, sent))
    swapped = merge(swapped, *others)
    hop = 8
    while hop < groups:
        swapped = merge(swapped, exchange(swapped, hop))
        hop *= 2
    lse, queue_copy, query = pl.pallas_call(
        functools.partial(early_kernel, images=images),
        out_shape=shapes + (pltpu.VMEM((count, kd), BF16),),
        in_specs=[whole, hbm],
        out_specs=(whole, hbm, whole),
        scratch_shapes=work,
        compiler_params=limit,
        name="early",
    )(hold(swapped), far(queue))
    lse, sent = lax.optimization_barrier((lse, sent))
    carry = lax.while_loop(lambda carry: carry[0][0] <= loops + 1, advance, (tick, came, sent, marks))
    _, came, sent, marks = carry
    coming = lax.ppermute(sent, "section", chain[-1:])
    marks = run_class(came, marks, weights, toks)
    came = coming

    lse, marks = lax.optimization_barrier((lse, marks))
    lse, queue_copy, window, owner_row, start = pl.pallas_call(
        late_kernel,
        out_shape=shapes
        + (
            pltpu.VMEM((32, kd), BF16),
            pltpu.VMEM((1, count), jnp.int32),
            pltpu.SMEM((1,), jnp.int32),
        ),
        in_specs=[whole, hbm, smem, whole, whole, hbm],
        out_specs=(whole, hbm, whole, whole, smem),
        scratch_shapes=work,
        input_output_aliases={5: 1},
        compiler_params=limit,
        name="late",
    )(hold(query), far(queue), pointer, owner.reshape(1, count), hold(lse), far(queue_copy))
    height = -(-(kd // LANES * images + 3 * extra) // 8) * 8
    message = pl.pallas_call(
        functools.partial(head_kernel, toks=toks),
        out_shape=jax.ShapeDtypeStruct((peers, height, LANES), BF16),
        in_specs=[whole] * 11,
        out_specs=whole,
        scratch_shapes=[
            pltpu.VMEM((images, width), F32),
            pltpu.VMEM((rows, width), BF16),
            pltpu.VMEM((rows, 3 * width), BF16),
            pltpu.VMEM((8, max(w_fc1.shape[2], width)), F32),
        ],
        compiler_params=pltpu.CompilerParams(vmem_limit_bytes=12 * 2**20),
        name="head",
    )(hold(came), hold(marks), *held_weights(weights), final_norm_gain.reshape(1, width), w_head, hold(lse))
    got = lax.all_to_all(message, ("dp", "section"), 0, 0, tiled=True)

    keys, loss, total, new_queue = pl.pallas_call(
        functools.partial(final_kernel, images=images, kd=kd),
        out_shape=(
            jax.ShapeDtypeStruct((images, kd), BF16),
            jax.ShapeDtypeStruct((1, images), F32),
            jax.ShapeDtypeStruct((1, 1), F32),
            jax.ShapeDtypeStruct(queue.shape, BF16),
        ),
        in_specs=[smem, whole, whole, whole, whole, hbm],
        out_specs=(whole, whole, whole, hbm),
        scratch_shapes=[pltpu.VMEM((32, kd), BF16), pltpu.SemaphoreType.DMA],
        input_output_aliases={5: 3},
        name="final",
    )(start, hold(got), hold(query), hold(owner_row), hold(window), far(queue_copy))
    return keys, loss.reshape(images), total.reshape(()), new_queue


def solution(mesh):
    placed = (
        P("dp", None, None),
        P("section", None),
        P("section", None, None),
        P("section", None, None),
        P("section", None),
        P("section", None, None),
        P("section", None, None),
        P(),
        P(),
        P("dp", None),
        P(("dp", "section"), None),
        P(),
        P("dp"),
    )
    return jax.shard_map(
        on_device,
        mesh=mesh,
        in_specs=placed,
        out_specs=(P("dp", None), P("dp"), P(), P(("dp", "section"), None)),
        check_vma=False,
    )
```
